32 devices in a mesh: aa: 8 (over y, x, core), ba: 4 (over z).
Axes of the slice: x: 2, y: 2, z: 4, core: 2. Of those that a mesh axis runs over, the one named last changes fastest.
Arguments:
- query: bfloat16 [3072, 4096], P('aa', 'ba'), may hold values from -28 to 28
- keys: bfloat16 [3072, 2048], P('aa', 'ba'), may hold values from -6 to 6
- values: bfloat16 [3072, 2048], P('aa', 'ba'), may hold values from -6 to 6
- grad_out: bfloat16 [3072, 5376], P('aa', 'ba'), may hold values from -6 to 6
- segment_ids: int32 [3072], P('aa'), may hold values from 0 to 5, never falling along the last dimension, each value on 1 to 1920 neighbouring positions
- w_query: bfloat16 [5376, 4096], P(None, 'ba'), may hold values from -0.125 to 0.125
- w_key: bfloat16 [5376, 2048], P(None, 'ba'), may hold values from -0.1875 to 0.1875
- w_value: bfloat16 [5376, 2048], P(None, 'ba'), may hold values from -0.1875 to 0.1875
- w_out: bfloat16 [4096, 5376], P('ba'), may hold values from -0.078125 to 0.078125
Outputs:
- grad_input: bfloat16 [3072, 5376], P('aa', 'ba')
The draws below stay inside these ranges and needn't reach their ends.
Inputs may be any that keep to these rules, and one draw needn't show every extreme that they name: `segment_ids`: never falls along the sequence; each document has at most 1920 positions.
All inputs are finite; a program needn't handle non-finite values.
Results may differ from the reference program's by a relative error of at most 0.019.
Values may be sent and summed in bfloat16 or wider, within the bound.
A program may use at most 128 MiB of HBM per device.

```python
import math
import jax
import jax.numpy as jnp
import numpy as np
from jax import lax

D = 5376
HQ = 32
KVH = 16
HD = 128
DOCS = 6
TOKENS = 3072
DOC_MOST = 1920


def query_key_pair(key):
    base = jax.random.fold_in(key, 4111)
    key_q, key_k = jax.random.split(base, 2)
    query = jax.random.truncated_normal(key_q, -6.0, 6.0, (TOKENS, KVH, 2, HD), jnp.float32)
    keys = jax.random.truncated_normal(key_k, -6.0, 6.0, (TOKENS, KVH, HD), jnp.float32)
    return (query.reshape(TOKENS, HQ * HD), keys.reshape(TOKENS, KVH * HD))


def draw_query(key, part):
    return query_key_pair(key)[0].astype(jnp.bfloat16)


def draw_keys(key, part):
    return query_key_pair(key)[1].astype(jnp.bfloat16)


def spiked(array, key, source, target, parts, factor):
    def block_of(dim):
        return (jnp.arange(array.shape[dim]) // (array.shape[dim] // parts)).reshape((-1,) + (1,) * (array.ndim - 1 - dim))

    first = jax.random.permutation(key, parts)[block_of(target)]
    far = (block_of(target) + parts // 2) % parts
    return jnp.where((block_of(source) == first) | (block_of(source) == far), factor * array, array)


def shard_levels(stream_key, dims, cuts, smallest, largest):
    def one(axis_at, blocks):
        heights = jax.random.uniform(jax.random.fold_in(jax.random.fold_in(stream_key, 6), axis_at), (blocks,), jnp.float32, smallest / len(cuts), largest / len(cuts))
        return jnp.repeat(jnp.exp(heights), dims[axis_at] // blocks).reshape((-1,) + (1,) * (len(dims) - axis_at - 1))

    gain = one(*cuts[0])
    for cut in cuts[1:]:
        gain = gain * one(*cut)
    return gain


def split_up(number_of, total, limit, lean):
    weights = [(1 << 20) // math.isqrt(rank ** lean) + 1 for rank in range(2, number_of + 1)]
    spare, counts = total - limit - (number_of - 1), [1] * (number_of - 1)
    while spare > 0:
        movable = [i for i in range(number_of - 1) if counts[i] < limit]
        pool, remaining = sum([weights[i] for i in movable]), spare
        for i in movable:
            extra = min(limit - counts[i], max(1, remaining * weights[i] // pool), spare)
            counts[i] = counts[i] + extra
            spare = spare - extra
    return np.array([limit] + counts)


def uneven_parts(own_key, amount, total, most, lean):
    if amount == 2:
        one = jax.random.randint(own_key, (), max(1, total - most), min(most, total - 1) + 1)
        return jnp.stack([one, total - one])
    tallies = jnp.asarray(split_up(amount, total, most, lean), jnp.int32)
    twos = (amount - 1) // 2
    giver, receiver = tallies[1:1 + 2 * twos:2], tallies[2:2 + 2 * twos:2]
    room = jnp.minimum(giver - 1, most - receiver)
    moved = jax.random.randint(jax.random.fold_in(own_key, 1), (twos,), 0, 1 << 20) % (room + 1)
    tallies = tallies.at[1:1 + 2 * twos:2].set(giver - moved).at[2:2 + 2 * twos:2].set(receiver + moved)
    return tallies[jax.random.permutation(jax.random.fold_in(own_key, 2), amount)]


def noise(own_key, extent, width, limit, cuts=(), held_as=jnp.bfloat16):
    drawn = jax.random.normal(own_key, extent, jnp.float32) * width
    if len(cuts) > 0:
        drawn = shard_levels(own_key, extent, cuts, -0.22, 0.18) * drawn
    return jnp.clip(drawn, min=-limit, max=limit).astype(held_as)


def noise_with(key, shape, width, reach, cuts, heavy, kind=jnp.bfloat16):
    entries = width * jax.random.normal(key, shape, jnp.float32)
    if cuts:
        entries = entries * shard_levels(key, shape, cuts, -0.22, 0.18)
    return jnp.clip(spiked(entries, jax.random.fold_in(key, 3), *heavy), -reach, reach).astype(kind)


def setup_inputs(seed: int = 0) -> dict:
    key_of = jax.random.split(jax.random.key(seed), 10)
    return {
        "query": draw_query(jax.random.fold_in(key_of[9], 71), 0),
        "keys": draw_keys(jax.random.fold_in(key_of[9], 71), 0),
        "values": noise(key_of[2], (TOKENS, KVH * HD), 1.0, 6.0, ((0, 8), (1, 4))),
        "grad_out": noise(key_of[3], (TOKENS, D), 1.0, 6.0, ((0, 8), (1, 4))),
        "segment_ids": jnp.searchsorted(jnp.cumsum(uneven_parts(key_of[4], DOCS, TOKENS, DOC_MOST, 1)), jnp.arange(TOKENS), side="right").astype(jnp.int32),
        "w_query": noise_with(key_of[5], (D, HQ * HD), (HQ * HD) ** -0.5, 0.125, ((1, 4),), (1, 0, 4, 2.0)),
        "w_key": noise_with(key_of[6], (D, KVH * HD), (KVH * HD) ** -0.5, 0.1875, ((1, 4),), (1, 0, 4, 2.0)),
        "w_value": noise_with(key_of[7], (D, KVH * HD), (KVH * HD) ** -0.5, 0.1875, ((1, 4),), (1, 0, 4, 2.0)),
        "w_out": noise(key_of[8], (HQ * HD, D), D ** -0.5, 0.078125, ((0, 4),)),
    }


NEG_FILL = -1e30


def back_project(grad, weight):
    return lax.dot_general(grad, weight, (((1,), (1,)), ((), ())), preferred_element_type=jnp.float32)


def reference(query, keys, values, grad_out, segment_ids, w_query, w_key, w_value, w_out):
    scaling = (D / HQ) ** -0.5
    dout = back_project(grad_out, w_out).astype(jnp.bfloat16)
    position = jnp.arange(TOKENS, dtype=jnp.int32)
    allowed = (position[None, :] <= position[:, None]) & (segment_ids[None, :] == segment_ids[:, None])
    query_grp = query.reshape(TOKENS, KVH, 2, HD).transpose(1, 0, 2, 3)
    dout_grp = dout.reshape(TOKENS, KVH, 2, HD).transpose(1, 0, 2, 3)
    keys_grp = keys.reshape(TOKENS, KVH, HD).transpose(1, 0, 2)
    values_grp = values.reshape(TOKENS, KVH, HD).transpose(1, 0, 2)
    highest = lax.Precision.HIGHEST

    def one_group(items):
        query_four, dout_four, key_three, value_three = items
        query_f = query_four.astype(jnp.float32)
        dout_f = dout_four.astype(jnp.float32)
        key_f = key_three.astype(jnp.float32)
        value_f = value_three.astype(jnp.float32)
        scores = jnp.einsum("igd,jd->gij", query_f, key_f, precision=highest) * scaling
        masked = jnp.where(allowed, scores, NEG_FILL)
        top_val = jnp.max(masked, axis=-1)
        expo = jnp.where(allowed, jnp.exp(scores - top_val[..., None]), 0.0)
        lse = top_val + jnp.log(jnp.sum(expo, axis=-1))
        probs = jnp.where(allowed, jnp.exp(scores - lse[..., None]), 0.0)
        dprobs = jnp.einsum("igd,jd->gij", dout_f, value_f, precision=highest)
        delta = jnp.sum(probs * dprobs, axis=-1)
        dscores = probs * (dprobs - delta[..., None])
        probs_low = lax.optimization_barrier(probs.astype(jnp.bfloat16)).astype(jnp.float32)
        dscores_low = lax.optimization_barrier(dscores.astype(jnp.bfloat16)).astype(jnp.float32)
        grad_v = jnp.einsum("gij,igd->jd", probs_low, dout_f, precision=highest)
        grad_k = jnp.einsum("gij,igd->jd", dscores_low, query_f, precision=highest) * scaling
        grad_q = jnp.einsum("gij,jd->igd", dscores_low, key_f, precision=highest) * scaling
        return grad_q, grad_k, grad_v

    grad_q, grad_k, grad_v = lax.map(one_group, (query_grp, dout_grp, keys_grp, values_grp))
    grad_q = grad_q.transpose(1, 0, 2, 3).reshape(TOKENS, HQ * HD).astype(jnp.bfloat16)
    grad_k = grad_k.transpose(1, 0, 2).reshape(TOKENS, KVH * HD).astype(jnp.bfloat16)
    grad_v = grad_v.transpose(1, 0, 2).reshape(TOKENS, KVH * HD).astype(jnp.bfloat16)
    total = back_project(grad_q, w_query) + back_project(grad_k, w_key) + back_project(grad_v, w_value)
    return total.astype(jnp.bfloat16)
```

```python
import functools

import jax
import jax.numpy as jnp
from jax import lax
from jax.experimental import pallas as pl
from jax.experimental.pallas import tpu as pltpu
from jax.sharding import PartitionSpec as P

D = 5376
HQ = 32
HD = 128
DOCS = 6


NEG_FILL = -1e30


def from_behind(value, axis, steps):
    count = lax.axis_size(axis)
    pairs = [(source, (source + steps) % count) for source in range(count)]
    return lax.ppermute(value, axis, pairs)


def block_scores(query, dout, keys, values, query_pos, query_seg, key_pos, key_seg, scaling):
    row_count = query.shape[0]
    col_count = keys.shape[0]
    groups = keys.shape[1] // HD
    query_four = query.reshape(row_count, groups, 2, HD)
    dout_four = dout.reshape(row_count, groups, 2, HD)
    key_three = keys.reshape(col_count, groups, HD)
    value_three = values.reshape(col_count, groups, HD)
    scores = (
        jnp.einsum("iagd,jad->agij", query_four, key_three, preferred_element_type=jnp.float32)
        * scaling
    )
    dprobs = jnp.einsum(
        "iagd,jad->agij", dout_four, value_three, preferred_element_type=jnp.float32
    )
    allowed = (key_pos[None, :] <= query_pos[:, None]) & (key_seg[None, :] == query_seg[:, None])
    return (scores, dprobs, allowed, query_four, dout_four, key_three)


def forward_stats(
    query, dout, keys, values, query_pos, query_seg, key_pos, key_seg, scaling, state
):
    run_max, run_sum, run_dot = state
    scores, dprobs, allowed, unused_q, unused_d, unused_k = block_scores(
        query, dout, keys, values, query_pos, query_seg, key_pos, key_seg, scaling
    )
    masked = jnp.where(allowed, scores, NEG_FILL)
    new_max = jnp.maximum(run_max, jnp.max(masked, axis=-1))
    expo = jnp.where(allowed, jnp.exp(scores - new_max[..., None]), 0.0)
    return (new_max, jnp.sum(expo, axis=-1), jnp.sum(expo * dprobs, axis=-1))


def block_grads(
    query, dout, row_lse, row_delta, keys, values, query_pos, query_seg, key_pos, key_seg, scaling
):
    scores, dprobs, allowed, query_four, dout_four, key_three = block_scores(
        query, dout, keys, values, query_pos, query_seg, key_pos, key_seg, scaling
    )
    softmax_w = jnp.where(allowed, jnp.exp(scores - row_lse[..., None]), 0.0)
    dscores = softmax_w * (dprobs - row_delta[..., None])
    softmax_low = softmax_w.astype(jnp.bfloat16)
    dscores_low = dscores.astype(jnp.bfloat16)
    grad_v = jnp.einsum(
        "agij,iagd->jad", softmax_low, dout_four, preferred_element_type=jnp.float32
    )
    grad_k = (
        jnp.einsum("agij,iagd->jad", dscores_low, query_four, preferred_element_type=jnp.float32)
        * scaling
    )
    grad_q = (
        jnp.einsum("agij,jad->iagd", dscores_low, key_three, preferred_element_type=jnp.float32)
        * scaling
    )
    return (
        grad_q.reshape(query.shape[0], -1),
        grad_k.reshape(keys.shape[0], -1),
        grad_v.reshape(keys.shape[0], -1),
    )


def project_back(grad, weight):
    return lax.dot_general(
        grad, weight, (((1,), (1,)), ((), ())), preferred_element_type=jnp.float32
    )


def local_ring(query, keys, values, grad_out, segment_ids, w_query, w_key, w_value, w_out):
    seq_devices = lax.axis_size("aa")
    own_index = lax.axis_index("aa")
    tok_count = query.shape[0]
    scaling = (D / HQ) ** (-0.5)
    groups = keys.shape[1] // HD
    all_seg = lax.all_gather(segment_ids, "aa", axis=0, tiled=True)
    dout = project_back(lax.all_gather(grad_out, "ba", axis=1, tiled=True), w_out).astype(
        jnp.bfloat16
    )
    offsets = lax.iota(jnp.int32, tok_count)
    own_pos = own_index * tok_count + offsets
    own_seg = lax.dynamic_slice_in_dim(all_seg, own_index * tok_count, tok_count)
    stat_shape = (groups, 2, tok_count)
    stats_start = (
        jnp.full(stat_shape, NEG_FILL, jnp.float32),
        jnp.zeros(stat_shape, jnp.float32),
        jnp.zeros(stat_shape, jnp.float32),
    )
    piece = (
        lax.all_gather(keys, "aa", axis=0, tiled=True),
        lax.all_gather(values, "aa", axis=0, tiled=True),
    )
    width = piece[0].shape[0]
    key_pos = lax.iota(jnp.int32, width)
    key_seg = all_seg
    run_max, run_sum, run_dot = forward_stats(
        query, dout, piece[0], piece[1], own_pos, own_seg, key_pos, key_seg, scaling, stats_start
    )
    row_lse = run_max + jnp.log(run_sum)
    row_delta = run_dot / run_sum
    zero_q = jnp.zeros(query.shape, jnp.float32)
    zero_k = jnp.zeros(keys.shape, jnp.float32)

    def step_keys(step_index, state):
        (keys_now, values_now), (dk_now, dv_now), grad_q = state
        anchor = (own_index - step_index) % seq_devices
        key_pos = anchor * tok_count + offsets
        key_seg = lax.dynamic_slice_in_dim(all_seg, anchor * tok_count, tok_count)
        add_q, add_k, add_v = block_grads(
            query,
            dout,
            row_lse,
            row_delta,
            keys_now,
            values_now,
            own_pos,
            own_seg,
            key_pos,
            key_seg,
            scaling,
        )
        bundle_next = from_behind((keys_now, values_now), "aa", 1)
        sums_next = (
            from_behind((dk_now + add_k).astype(jnp.bfloat16), "aa", 1).astype(jnp.float32),
            from_behind((dv_now + add_v).astype(jnp.bfloat16), "aa", 1).astype(jnp.float32),
        )
        return (bundle_next, sums_next, grad_q + add_q)

    initial = ((keys, values), (zero_k, zero_k), zero_q)
    final = lax.fori_loop(0, seq_devices, step_keys, initial)
    grad_q = final[2]
    grad_k = final[1][0]
    grad_v = final[1][1]
    partial_value = (
        project_back(grad_q.astype(jnp.bfloat16), w_query)
        + project_back(grad_k.astype(jnp.bfloat16), w_key)
        + project_back(grad_v.astype(jnp.bfloat16), w_value)
    )
    return lax.psum_scatter(
        partial_value.astype(jnp.bfloat16), "ba", scatter_dimension=1, tiled=True
    )


def fold_rows(value, op):
    return op(value.reshape(-1, 8, value.shape[1]), axis=0)


CONTRACT_LAST = (((1,), (1,)), ((), ()))


WHOLE = pl.BlockSpec(memory_space=pltpu.VMEM)


MESH = pl.DeviceIdType.MESH
HBM = pl.BlockSpec(memory_space=pl.ANY)
SUBS = 3


def scatter_kernel(planes, gq_ref, gkv_ref, wq_ref, wk_ref, wv_ref, out_ref, wqb, wkb, wvb, sbuf, rbuf, total_ref, wsem, ssem, rsem):
    z = lax.axis_index("ba")
    barrier = pltpu.get_barrier_semaphore()
    last = planes - 1
    low = z > 0
    high = z < last

    @pl.when(low)
    def _():
        pl.semaphore_signal(barrier, inc=1, device_id={"ba": z - 1}, device_id_type=MESH)

    @pl.when(high)
    def _():
        pl.semaphore_signal(barrier, inc=1, device_id={"ba": z + 1}, device_id_type=MESH)

    rows = out_ref.shape[0]
    sub_rows = rows // SUBS

    def target(side, step):
        return step if side == 0 else last - step

    def sends(side, step):
        return step < z if side == 0 else step < last - z

    def weight_copies(feature, slot):
        span = pl.ds(pl.multiple_of(feature * rows, 16), rows)
        return [
            pltpu.make_async_copy(src.at[span], dst.at[slot], wsem.at[slot, part])
            for part, (src, dst) in enumerate(((wq_ref, wqb), (wk_ref, wkb), (wv_ref, wvb)))
        ]

    order = [(step, side) for step in range(last) for side in range(2)]

    def slot_of(side, step):
        return step if side == 0 else last - step

    for step, side in order:
        @pl.when(sends(side, step))
        def _(step=step, side=side):
            for copy in weight_copies(target(side, step), slot_of(side, step)):
                copy.start()
    for copy in weight_copies(z, z):
        copy.start()

    pl.semaphore_wait(barrier, jnp.minimum(z, 1) + jnp.minimum(last - z, 1))

    half = gkv_ref.shape[1] // 2

    def part(slot, sub):
        span = pl.ds(sub * sub_rows, sub_rows)
        acc = jnp.dot(wqb[slot, span, :], gq_ref[...], preferred_element_type=jnp.float32)
        acc += lax.dot_general(wkb[slot, span, :], gkv_ref[:, 0:half], CONTRACT_LAST, preferred_element_type=jnp.float32)
        return acc + lax.dot_general(wvb[slot, span, :], gkv_ref[:, half:], CONTRACT_LAST, preferred_element_type=jnp.float32)

    def hop(side, step, sub):
        span = pl.ds(sub * sub_rows, sub_rows)
        return pltpu.make_async_remote_copy(
            src_ref=sbuf.at[side, step, span],
            dst_ref=rbuf.at[side, step, span],
            send_sem=ssem.at[side, step, sub],
            recv_sem=rsem.at[side, step, sub],
            device_id={"ba": z - 1 if side == 0 else z + 1},
            device_id_type=MESH,
        )

    for step, side in order:
        behind = high if side == 0 else low

        @pl.when(sends(side, step))
        def _(step=step, side=side, behind=behind):
            slot = slot_of(side, step)
            for copy in weight_copies(target(side, step), slot):
                copy.wait()
            for sub in range(SUBS):
                span = pl.ds(sub * sub_rows, sub_rows)
                acc = part(slot, sub)

                @pl.when(behind)
                def _():
                    hop(side, step, sub).wait_recv()
                    sbuf[side, step, span, :] = (acc + rbuf[side, step, span, :].astype(jnp.float32)).astype(jnp.bfloat16)

                @pl.when(jnp.logical_not(behind))
                def _():
                    sbuf[side, step, span, :] = acc.astype(jnp.bfloat16)

                hop(side, step, sub).start()

    for copy in weight_copies(z, z):
        copy.wait()
    for sub in range(SUBS):
        span = pl.ds(sub * sub_rows, sub_rows)
        total_ref[span, :] = part(z, sub)
    for sub in range(SUBS):
        span = pl.ds(sub * sub_rows, sub_rows)
        for side in range(2):
            for step in range(last):
                here = (z == target(side, step)) & (high if side == 0 else low)

                @pl.when(here)
                def _(side=side, step=step):
                    hop(side, step, sub).wait_recv()
                    total_ref[span, :] += rbuf[side, step, span, :].astype(jnp.float32)

        out_ref[span, :] = total_ref[span, :].astype(jnp.bfloat16)

    for step, side in order:
        @pl.when(sends(side, step))
        def _(step=step, side=side):
            for sub in range(SUBS):
                hop(side, step, sub).wait_send()


def project_scatter(gq, gkv, w_query, w_key, w_value):
    planes = lax.axis_size("ba")
    rows = w_query.shape[0] // planes
    tokens = gq.shape[1]
    last = planes - 1
    return pl.pallas_call(
        functools.partial(scatter_kernel, planes),
        out_shape=jax.ShapeDtypeStruct((rows, tokens), jnp.bfloat16),
        in_specs=[WHOLE, WHOLE, HBM, HBM, HBM],
        out_specs=WHOLE,
        scratch_shapes=[
            pltpu.VMEM((planes, rows, w_query.shape[1]), jnp.bfloat16),
            pltpu.VMEM((planes, rows, w_key.shape[1]), jnp.bfloat16),
            pltpu.VMEM((planes, rows, w_value.shape[1]), jnp.bfloat16),
            pltpu.VMEM((2, last, rows, tokens), jnp.bfloat16),
            pltpu.VMEM((2, last, rows, tokens), jnp.bfloat16),
            pltpu.VMEM((rows, tokens), jnp.float32),
            pltpu.SemaphoreType.DMA((planes, 3)),
            pltpu.SemaphoreType.DMA((2, last, SUBS)),
            pltpu.SemaphoreType.DMA((2, last, SUBS)),
        ],
        compiler_params=pltpu.CompilerParams(
            collective_id=1, has_side_effects=True, vmem_limit_bytes=56 * 1024 * 1024
        ),
        name="project_scatter",
    )(gq, gkv, w_query, w_key, w_value)


CHUNK = 128
LOG2E = 1.4426950408889634


def attention_kernel(peers, planes, chunks, scaling, q_ref, k_ref, v_ref, seg_ref, g_ref, w_ref, gq_ref, gkv_ref,
                     wbuf, fbuf, qa, ka, va, kt, vt, segs, starts_ref, s_ref, p_ref, ot_ref, inv_ref, dvk_ref,
                     dsend, drecv, gqs, pair_out, pair_in, kvs,
                     local_sem, own_sem, ag_s, ag_r, x_s, x_r, d_s, d_r, gq_s, gq_r, pr_s, pr_r, kv_s, kv_r):
    me = lax.axis_index("aa")
    z = lax.axis_index("ba")
    last = planes - 1
    tok = q_ref.shape[0]
    feats = g_ref.shape[0]
    half = gkv_ref.shape[1] // 2
    barrier = pltpu.get_barrier_semaphore()

    def lanes(index):
        return pl.ds(pl.multiple_of(index * HD, HD), HD)

    def rows_of(index):
        return pl.ds(pl.multiple_of(index * tok, tok), tok)

    def peer(r):
        return lax.rem(me + r, peers)

    for r in range(1, peers):
        pl.semaphore_signal(barrier, inc=1, device_id={"aa": peer(r)}, device_id_type=MESH)
    for r in range(1, planes):
        pl.semaphore_signal(barrier, inc=1, device_id={"ba": lax.rem(z + r, planes)}, device_id_type=MESH)

    def own_copies():
        return [
            pltpu.make_async_copy(g_ref, fbuf.at[pl.ds(pl.multiple_of(z * feats, 16), feats)], own_sem.at[0]),
            pltpu.make_async_copy(q_ref.at[:, lanes(me)], qa.at[rows_of(me)], own_sem.at[1]),
            pltpu.make_async_copy(k_ref.at[:, lanes(me // 2)], ka.at[rows_of(me)], own_sem.at[2]),
            pltpu.make_async_copy(v_ref.at[:, lanes(me // 2)], va.at[rows_of(me)], own_sem.at[3]),
            pltpu.make_async_copy(seg_ref, segs.at[me], own_sem.at[4]),
        ]

    weight_copy = pltpu.make_async_copy(w_ref, wbuf, local_sem)
    for copy in own_copies():
        copy.start()
    pl.semaphore_wait(barrier, peers + planes - 2)

    def gather(side, c, s):
        source = z - s if side == 0 else z + s
        span = pl.ds(pl.multiple_of(source * feats, 16), feats)
        cols = pl.ds(c * CHUNK, CHUNK)
        return pltpu.make_async_remote_copy(
            src_ref=g_ref.at[:, cols] if s == 0 else fbuf.at[span, cols],
            dst_ref=fbuf.at[span, cols],
            send_sem=ag_s.at[side, c, s],
            recv_sem=ag_r.at[side, c, s],
            device_id={"ba": z + 1 if side == 0 else z - 1},
            device_id_type=MESH,
        )

    def arrival(side, c, s):
        source = z - 1 - s if side == 0 else z + 1 + s
        span = pl.ds(pl.multiple_of(source * feats, 16), feats)
        cols = pl.ds(c * CHUNK, CHUNK)
        return pltpu.make_async_remote_copy(
            src_ref=fbuf.at[span, cols],
            dst_ref=fbuf.at[span, cols],
            send_sem=ag_s.at[side, c, s],
            recv_sem=ag_r.at[side, c, s],
            device_id={"ba": z + 1 if side == 0 else z - 1},
            device_id_type=MESH,
        )

    def gather_sends(side, s):
        return (z >= s) & (z < last) if side == 0 else (z + s <= last) & (z > 0)

    def relay(c, s):
        for side in range(2):
            @pl.when(gather_sends(side, s))
            def _(side=side):
                if s > 0:
                    arrival(side, c, s - 1).wait_recv()
                gather(side, c, s).start()

    def finish_gather(c):
        for side in range(2):
            for s in range(last):
                @pl.when((z == last) if side == 0 else (z == 0))
                def _(side=side, s=s):
                    arrival(side, c, s).wait_recv()

    def exchange(kind, to, sender, peer_sem):
        shard = (q_ref.at[:, lanes(to)], k_ref.at[:, lanes(to // 2)], v_ref.at[:, lanes(to // 2)], seg_ref)[kind]
        land = (qa.at[rows_of(sender)], ka.at[rows_of(sender)], va.at[rows_of(sender)], segs.at[sender])[kind]
        return pltpu.make_async_remote_copy(
            src_ref=shard,
            dst_ref=land,
            send_sem=x_s.at[kind, peer_sem],
            recv_sem=x_r.at[kind, sender],
            device_id={"aa": to},
            device_id_type=MESH,
        )

    relay(0, 0)
    relay(1, 0)
    for r in range(1, peers):
        exchange(3, peer(r), me, r).start()
    for r in range(1, peers):
        for kind in range(3):
            exchange(kind, peer(r), me, r).start()
    weight_copy.start()
    dvk_ref[...] = jnp.zeros_like(dvk_ref)
    relay(0, 1)
    relay(1, 1)
    for copy in own_copies():
        copy.wait()
    for r in range(1, peers):
        exchange(3, me, peer(r), r).wait_recv()

    ids = segs[...]
    starts = jnp.zeros(ids.shape, jnp.float32)
    for doc in range(1, DOCS):
        before = jnp.sum(jnp.where(ids < doc, 1.0, 0.0), axis=(0, 2), keepdims=True)
        starts = jnp.where(ids == doc, before, starts)
    starts_ref[...] = starts
    relay(0, 2)
    relay(2, 0)

    def tri(m):
        return m * (m + 1) // 2 * CHUNK

    def stats(c, first):
        def block(a, carry):
            m = chunks * a + c
            if first:
                @pl.when(a != me)
                def _():
                    for kind in range(3):
                        exchange(kind, me, a, 0).wait_recv()

                kt[:, rows_of(a)] = ka[rows_of(a), :].astype(jnp.float32).T.astype(jnp.bfloat16)
                vt[:, rows_of(a)] = va[rows_of(a), :].astype(jnp.float32).T.astype(jnp.bfloat16)
            query = qa[pl.ds(pl.multiple_of(m * CHUNK, CHUNK), CHUNK), :]
            begin = starts_ref[a, :, c * CHUNK : (c + 1) * CHUNK]

            def scores(at, size, diagonal):
                span = pl.ds(pl.multiple_of(at, CHUNK), size)
                s = lax.dot_general(ka[span, :], query, CONTRACT_LAST, preferred_element_type=jnp.float32)
                key = lax.broadcasted_iota(jnp.int32, (size, CHUNK), 0)
                if diagonal:
                    allowed = key <= c * CHUNK + lax.broadcasted_iota(jnp.int32, (size, CHUNK), 1)
                    allowed &= (key + at).astype(jnp.float32) >= begin
                else:
                    allowed = (key + at).astype(jnp.float32) >= begin
                s = jnp.where(allowed, s * (scaling * LOG2E), NEG_FILL)
                s_ref[span, :] = s
                return fold_rows(s, jnp.max)

            top = lax.fori_loop(0, a, lambda u, t: jnp.maximum(t, scores(u * tok, tok, False)),
                                jnp.full((8, CHUNK), NEG_FILL, jnp.float32))
            size = (c + 1) * CHUNK
            top = jnp.maximum(top, scores(a * tok, size, True))
            top = jnp.max(top, axis=0, keepdims=True)

            def weights(at, size, state):
                total, out = state
                span = pl.ds(pl.multiple_of(at, CHUNK), size)
                p = jnp.exp2(s_ref[span, :] - top)
                low = p.astype(jnp.bfloat16)
                p_ref[pl.ds(pl.multiple_of(tri(m) + at, CHUNK), size), :] = low
                return (total + fold_rows(p, jnp.sum),
                        out + jnp.dot(vt[:, span], low, preferred_element_type=jnp.float32))

            state = (jnp.zeros((8, CHUNK), jnp.float32), jnp.zeros((HD, CHUNK), jnp.float32))
            state = lax.fori_loop(0, a, lambda u, st: weights(u * tok, tok, st), state)
            total, out = weights(a * tok, size, state)
            inverse = 1.0 / jnp.sum(total, axis=0, keepdims=True)
            inv_ref[m] = inverse
            ot_ref[m] = out * inverse
            return carry

        lax.fori_loop(0, peers, block, 0)

    def dout_send(c, to):
        return pltpu.make_async_remote_copy(
            src_ref=dsend.at[c, to],
            dst_ref=drecv.at[c, me],
            send_sem=d_s.at[c, to],
            recv_sem=d_r.at[c, me],
            device_id={"aa": to},
            device_id_type=MESH,
        )

    def dout_arrival(c, sender):
        return pltpu.make_async_remote_copy(
            src_ref=dsend.at[c, sender],
            dst_ref=drecv.at[c, sender],
            send_sem=d_s.at[c, sender],
            recv_sem=d_r.at[c, sender],
            device_id={"aa": sender},
            device_id_type=MESH,
        )

    def project(c):
        finish_gather(c)
        pair = 2

        def heads(i, carry):
            span = pl.ds(pl.multiple_of(i * (pair * HD), HD), pair * HD)
            out = jnp.dot(wbuf[span, :], fbuf[:, c * CHUNK : (c + 1) * CHUNK], preferred_element_type=jnp.float32)
            for j in range(pair):
                to = i * pair + j
                dsend[c, to] = out[j * HD : (j + 1) * HD, :].astype(jnp.bfloat16)

                @pl.when(to != me)
                def _():
                    dout_send(c, to).start()

            return carry

        lax.fori_loop(0, peers // pair, heads, 0)
        drecv[c, me] = dsend[c, me]

    def gq_copy(c, to):
        return pltpu.make_async_remote_copy(
            src_ref=gqs.at[c, to],
            dst_ref=gq_ref.at[lanes(me), pl.ds(c * CHUNK, CHUNK)],
            send_sem=gq_s.at[c, to],
            recv_sem=gq_r.at[c, me],
            device_id={"aa": to},
            device_id_type=MESH,
        )

    def gq_arrival(c, sender):
        return pltpu.make_async_remote_copy(
            src_ref=gqs.at[c, sender],
            dst_ref=gq_ref.at[lanes(sender), pl.ds(c * CHUNK, CHUNK)],
            send_sem=gq_s.at[c, sender],
            recv_sem=gq_r.at[c, sender],
            device_id={"aa": sender},
            device_id_type=MESH,
        )

    def gq_local(c):
        return pltpu.make_async_copy(gqs.at[c, me], gq_ref.at[lanes(me), pl.ds(c * CHUNK, CHUNK)], own_sem.at[c])

    def grads(c):
        def block(a, carry):
            m = chunks * a + c

            @pl.when(a != me)
            def _():
                dout_arrival(c, a).wait_recv()

            query = qa[pl.ds(pl.multiple_of(m * CHUNK, CHUNK), CHUNK), :]
            dout = (drecv[c, a].astype(jnp.float32) * inv_ref[m]).astype(jnp.bfloat16)
            delta = jnp.sum(dout.astype(jnp.float32) * ot_ref[m], axis=0, keepdims=True)

            def unit(at, size, grad_q):
                span = pl.ds(pl.multiple_of(at, CHUNK), size)
                p = p_ref[pl.ds(pl.multiple_of(tri(m) + at, CHUNK), size), :]
                dp = jnp.dot(va[span, :], dout, preferred_element_type=jnp.float32)
                ds = (p.astype(jnp.float32) * (dp - delta)).astype(jnp.bfloat16)
                dvk_ref[span, 0:HD] += lax.dot_general(p, dout, CONTRACT_LAST, preferred_element_type=jnp.float32)
                dvk_ref[span, HD:] += jnp.dot(ds, query, preferred_element_type=jnp.float32)
                return grad_q + jnp.dot(kt[:, span], ds, preferred_element_type=jnp.float32)

            grad_q = lax.fori_loop(0, a, lambda u, t: unit(u * tok, tok, t), jnp.zeros((HD, CHUNK), jnp.float32))
            grad_q = unit(a * tok, (c + 1) * CHUNK, grad_q)
            gqs[c, a] = (grad_q * scaling).astype(jnp.bfloat16)

            @pl.when(a != me)
            def _():
                gq_copy(c, a).start()

            return carry

        lax.fori_loop(0, peers, block, 0)
        gq_local(c).start()

    stats(0, True)
    relay(1, 2)
    stats(1, False)
    relay(2, 1)
    weight_copy.wait()
    project(0)
    stats(2, False)
    relay(2, 2)
    project(1)
    grads(0)
    grads(1)
    project(2)
    grads(2)

    odd = lax.rem(me, 2)
    partner = me + 1 - 2 * odd
    pair_copy = pltpu.make_async_remote_copy(
        src_ref=pair_out, dst_ref=pair_in, send_sem=pr_s, recv_sem=pr_r, device_id={"aa": partner}, device_id_type=MESH
    )

    @pl.when(odd == 0)
    def _():
        pair_out[...] = dvk_ref[:, 0:HD].astype(jnp.bfloat16)

    @pl.when(odd == 1)
    def _():
        pair_out[...] = (dvk_ref[:, HD:] * scaling).astype(jnp.bfloat16)

    pair_copy.start()
    pair_copy.wait_recv()

    @pl.when(odd == 0)
    def _():
        kvs[...] = (dvk_ref[:, HD:] * scaling + pair_in[...].astype(jnp.float32)).astype(jnp.bfloat16)

    @pl.when(odd == 1)
    def _():
        kvs[...] = (dvk_ref[:, 0:HD] + pair_in[...].astype(jnp.float32)).astype(jnp.bfloat16)

    def kv_cols(sender):
        return pl.ds(pl.multiple_of(lax.rem(sender, 2) * half + sender // 2 * HD, HD), HD)

    def kv_copy(to):
        return pltpu.make_async_remote_copy(
            src_ref=kvs.at[rows_of(to)],
            dst_ref=gkv_ref.at[:, kv_cols(me)],
            send_sem=kv_s.at[to],
            recv_sem=kv_r.at[me],
            device_id={"aa": to},
            device_id_type=MESH,
        )

    def kv_arrival(sender):
        return pltpu.make_async_remote_copy(
            src_ref=kvs.at[rows_of(sender)],
            dst_ref=gkv_ref.at[:, kv_cols(sender)],
            send_sem=kv_s.at[sender],
            recv_sem=kv_r.at[sender],
            device_id={"aa": sender},
            device_id_type=MESH,
        )

    for r in range(1, peers):
        kv_copy(peer(r)).start()
    kv_local = pltpu.make_async_copy(kvs.at[rows_of(me)], gkv_ref.at[:, kv_cols(me)], own_sem.at[3])
    kv_local.start()

    for c in range(chunks):
        gq_local(c).wait()
    kv_local.wait()
    for r in range(1, peers):
        other = peer(r)
        for c in range(chunks):
            gq_arrival(c, other).wait_recv()
        kv_arrival(other).wait_recv()
    for r in range(1, peers):
        other = peer(r)
        for kind in range(4):
            exchange(kind, other, me, r).wait_send()
        for c in range(chunks):
            dout_send(c, other).wait_send()
            gq_copy(c, other).wait_send()
        kv_copy(other).wait_send()
    pair_copy.wait_send()
    for side in range(2):
        for s in range(last):
            @pl.when(gather_sends(side, s))
            def _(side=side, s=s):
                for c in range(chunks):
                    gather(side, c, s).wait_send()


def attention_grads(query, keys, values, segment_ids, grad_out, w_out, scaling):
    peers, planes = lax.axis_size("aa"), lax.axis_size("ba")
    tok = query.shape[0]
    chunks = tok // CHUNK
    total = peers * tok
    blocks = peers * chunks
    low, full = jnp.bfloat16, jnp.float32
    return pl.pallas_call(
        functools.partial(attention_kernel, peers, planes, chunks, scaling),
        out_shape=[
            jax.ShapeDtypeStruct((query.shape[1], tok), low),
            jax.ShapeDtypeStruct((tok, 2 * keys.shape[1]), low),
        ],
        in_specs=[HBM] * 6,
        out_specs=[WHOLE, WHOLE],
        scratch_shapes=[
            pltpu.VMEM(w_out.shape, low),
            pltpu.VMEM((w_out.shape[1], tok), low),
            pltpu.VMEM((total, HD), low),
            pltpu.VMEM((total, HD), low),
            pltpu.VMEM((total, HD), low),
            pltpu.VMEM((HD, total), low),
            pltpu.VMEM((HD, total), low),
            pltpu.VMEM((peers, 1, tok), jnp.int32),
            pltpu.VMEM((peers, 1, tok), full),
            pltpu.VMEM((total, CHUNK), full),
            pltpu.VMEM((blocks * (blocks + 1) // 2 * CHUNK, CHUNK), low),
            pltpu.VMEM((blocks, HD, CHUNK), full),
            pltpu.VMEM((blocks, 1, CHUNK), full),
            pltpu.VMEM((total, 2 * HD), full),
            pltpu.VMEM((chunks, peers, HD, CHUNK), low),
            pltpu.VMEM((chunks, peers, HD, CHUNK), low),
            pltpu.VMEM((chunks, peers, HD, CHUNK), low),
            pltpu.VMEM((total, HD), low),
            pltpu.VMEM((total, HD), low),
            pltpu.VMEM((total, HD), low),
            pltpu.SemaphoreType.DMA,
            pltpu.SemaphoreType.DMA((5,)),
            pltpu.SemaphoreType.DMA((2, chunks, planes - 1)),
            pltpu.SemaphoreType.DMA((2, chunks, planes - 1)),
            pltpu.SemaphoreType.DMA((4, peers)),
            pltpu.SemaphoreType.DMA((4, peers)),
            pltpu.SemaphoreType.DMA((chunks, peers)),
            pltpu.SemaphoreType.DMA((chunks, peers)),
            pltpu.SemaphoreType.DMA((chunks, peers)),
            pltpu.SemaphoreType.DMA((chunks, peers)),
            pltpu.SemaphoreType.DMA,
            pltpu.SemaphoreType.DMA,
            pltpu.SemaphoreType.DMA((peers,)),
            pltpu.SemaphoreType.DMA((peers,)),
        ],
        compiler_params=pltpu.CompilerParams(
            collective_id=0, has_side_effects=True, vmem_limit_bytes=60 * 1024 * 1024
        ),
        name="attention_grads",
    )(query, keys, values, segment_ids.reshape(1, -1), grad_out.T, w_out)


def local(query, keys, values, grad_out, segment_ids, w_query, w_key, w_value, w_out):
    seq_devices, planes = lax.axis_size("aa"), lax.axis_size("ba")
    heads, groups = query.shape[1] // HD, keys.shape[1] // HD
    fits = heads == seq_devices and 2 * groups == heads and planes == 4 and query.shape[0] == 3 * CHUNK
    if not fits:
        return local_ring(query, keys, values, grad_out, segment_ids, w_query, w_key, w_value, w_out)
    scaling = (D / HQ) ** (-0.5)
    grad_q, grad_kv = attention_grads(query, keys, values, segment_ids, grad_out, w_out, scaling)
    return project_scatter(grad_q, grad_kv, w_query, w_key, w_value).T


def solution(mesh):
    return jax.shard_map(
        local,
        mesh=mesh,
        in_specs=(
            P("aa", "ba"),
            P("aa", "ba"),
            P("aa", "ba"),
            P("aa", "ba"),
            P("aa"),
            P(None, "ba"),
            P(None, "ba"),
            P(None, "ba"),
            P("ba", None),
        ),
        out_specs=P("aa", "ba"),
        check_vma=False,
    )
```

```python
import functools

import jax
import jax.numpy as jnp
from jax import lax
from jax.experimental import pallas as pl
from jax.experimental.pallas import tpu as pltpu
from jax.sharding import PartitionSpec as P

D = 5376
HQ = 32
HD = 128
DOCS = 6


NEG_FILL = -1e30


def from_behind(value, axis, steps):
    count = lax.axis_size(axis)
    pairs = [(source, (source + steps) % count) for source in range(count)]
    return lax.ppermute(value, axis, pairs)


def block_scores(query, dout, keys, values, query_pos, query_seg, key_pos, key_seg, scaling):
    row_count = query.shape[0]
    col_count = keys.shape[0]
    groups = keys.shape[1] // HD
    query_four = query.reshape(row_count, groups, 2, HD)
    dout_four = dout.reshape(row_count, groups, 2, HD)
    key_three = keys.reshape(col_count, groups, HD)
    value_three = values.reshape(col_count, groups, HD)
    scores = (
        jnp.einsum("iagd,jad->agij", query_four, key_three, preferred_element_type=jnp.float32)
        * scaling
    )
    dprobs = jnp.einsum(
        "iagd,jad->agij", dout_four, value_three, preferred_element_type=jnp.float32
    )
    allowed = (key_pos[None, :] <= query_pos[:, None]) & (key_seg[None, :] == query_seg[:, None])
    return (scores, dprobs, allowed, query_four, dout_four, key_three)


def forward_stats(
    query, dout, keys, values, query_pos, query_seg, key_pos, key_seg, scaling, state
):
    run_max, run_sum, run_dot = state
    scores, dprobs, allowed, unused_q, unused_d, unused_k = block_scores(
        query, dout, keys, values, query_pos, query_seg, key_pos, key_seg, scaling
    )
    masked = jnp.where(allowed, scores, NEG_FILL)
    new_max = jnp.maximum(run_max, jnp.max(masked, axis=-1))
    expo = jnp.where(allowed, jnp.exp(scores - new_max[..., None]), 0.0)
    return (new_max, jnp.sum(expo, axis=-1), jnp.sum(expo * dprobs, axis=-1))


def block_grads(
    query, dout, row_lse, row_delta, keys, values, query_pos, query_seg, key_pos, key_seg, scaling
):
    scores, dprobs, allowed, query_four, dout_four, key_three = block_scores(
        query, dout, keys, values, query_pos, query_seg, key_pos, key_seg, scaling
    )
    softmax_w = jnp.where(allowed, jnp.exp(scores - row_lse[..., None]), 0.0)
    dscores = softmax_w * (dprobs - row_delta[..., None])
    softmax_low = softmax_w.astype(jnp.bfloat16)
    dscores_low = dscores.astype(jnp.bfloat16)
    grad_v = jnp.einsum(
        "agij,iagd->jad", softmax_low, dout_four, preferred_element_type=jnp.float32
    )
    grad_k = (
        jnp.einsum("agij,iagd->jad", dscores_low, query_four, preferred_element_type=jnp.float32)
        * scaling
    )
    grad_q = (
        jnp.einsum("agij,jad->iagd", dscores_low, key_three, preferred_element_type=jnp.float32)
        * scaling
    )
    return (
        grad_q.reshape(query.shape[0], -1),
        grad_k.reshape(keys.shape[0], -1),
        grad_v.reshape(keys.shape[0], -1),
    )


def project_back(grad, weight):
    return lax.dot_general(
        grad, weight, (((1,), (1,)), ((), ())), preferred_element_type=jnp.float32
    )


def local_ring(query, keys, values, grad_out, segment_ids, w_query, w_key, w_value, w_out):
    seq_devices = lax.axis_size("aa")
    own_index = lax.axis_index("aa")
    tok_count = query.shape[0]
    scaling = (D / HQ) ** (-0.5)
    groups = keys.shape[1] // HD
    all_seg = lax.all_gather(segment_ids, "aa", axis=0, tiled=True)
    dout = project_back(lax.all_gather(grad_out, "ba", axis=1, tiled=True), w_out).astype(
        jnp.bfloat16
    )
    offsets = lax.iota(jnp.int32, tok_count)
    own_pos = own_index * tok_count + offsets
    own_seg = lax.dynamic_slice_in_dim(all_seg, own_index * tok_count, tok_count)
    stat_shape = (groups, 2, tok_count)
    stats_start = (
        jnp.full(stat_shape, NEG_FILL, jnp.float32),
        jnp.zeros(stat_shape, jnp.float32),
        jnp.zeros(stat_shape, jnp.float32),
    )
    piece = (
        lax.all_gather(keys, "aa", axis=0, tiled=True),
        lax.all_gather(values, "aa", axis=0, tiled=True),
    )
    width = piece[0].shape[0]
    key_pos = lax.iota(jnp.int32, width)
    key_seg = all_seg
    run_max, run_sum, run_dot = forward_stats(
        query, dout, piece[0], piece[1], own_pos, own_seg, key_pos, key_seg, scaling, stats_start
    )
    row_lse = run_max + jnp.log(run_sum)
    row_delta = run_dot / run_sum
    zero_q = jnp.zeros(query.shape, jnp.float32)
    zero_k = jnp.zeros(keys.shape, jnp.float32)

    def step_keys(step_index, state):
        (keys_now, values_now), (dk_now, dv_now), grad_q = state
        anchor = (own_index - step_index) % seq_devices
        key_pos = anchor * tok_count + offsets
        key_seg = lax.dynamic_slice_in_dim(all_seg, anchor * tok_count, tok_count)
        add_q, add_k, add_v = block_grads(
            query,
            dout,
            row_lse,
            row_delta,
            keys_now,
            values_now,
            own_pos,
            own_seg,
            key_pos,
            key_seg,
            scaling,
        )
        bundle_next = from_behind((keys_now, values_now), "aa", 1)
        sums_next = (
            from_behind((dk_now + add_k).astype(jnp.bfloat16), "aa", 1).astype(jnp.float32),
            from_behind((dv_now + add_v).astype(jnp.bfloat16), "aa", 1).astype(jnp.float32),
        )
        return (bundle_next, sums_next, grad_q + add_q)

    initial = ((keys, values), (zero_k, zero_k), zero_q)
    final = lax.fori_loop(0, seq_devices, step_keys, initial)
    grad_q = final[2]
    grad_k = final[1][0]
    grad_v = final[1][1]
    partial_value = (
        project_back(grad_q.astype(jnp.bfloat16), w_query)
        + project_back(grad_k.astype(jnp.bfloat16), w_key)
        + project_back(grad_v.astype(jnp.bfloat16), w_value)
    )
    return lax.psum_scatter(
        partial_value.astype(jnp.bfloat16), "ba", scatter_dimension=1, tiled=True
    )


def fold_rows(value, op):
    return op(value.reshape(-1, 8, value.shape[1]), axis=0)


CONTRACT_LAST = (((1,), (1,)), ((), ()))


WHOLE = pl.BlockSpec(memory_space=pltpu.VMEM)


MESH = pl.DeviceIdType.MESH
HBM = pl.BlockSpec(memory_space=pl.ANY)
SUBS = 3


def scatter_kernel(planes, gq_ref, gkv_ref, wq_ref, wk_ref, wv_ref, out_ref, wqb, wkb, wvb, sbuf, rbuf, total_ref, wsem, ssem, rsem):
    z = lax.axis_index("ba")
    barrier = pltpu.get_barrier_semaphore()
    last = planes - 1
    low = z > 0
    high = z < last

    @pl.when(low)
    def _():
        pl.semaphore_signal(barrier, inc=1, device_id={"ba": z - 1}, device_id_type=MESH)

    @pl.when(high)
    def _():
        pl.semaphore_signal(barrier, inc=1, device_id={"ba": z + 1}, device_id_type=MESH)

    rows = out_ref.shape[0]
    sub_rows = rows // SUBS

    def target(side, step):
        return step if side == 0 else last - step

    def sends(side, step):
        return step < z if side == 0 else step < last - z

    def weight_copies(feature, slot):
        span = pl.ds(pl.multiple_of(feature * rows, 16), rows)
        return [
            pltpu.make_async_copy(src.at[span], dst.at[slot], wsem.at[slot, part])
            for part, (src, dst) in enumerate(((wq_ref, wqb), (wk_ref, wkb), (wv_ref, wvb)))
        ]

    order = [(step, side) for step in range(last) for side in range(2)]

    def slot_of(side, step):
        return step if side == 0 else last - step

    for step, side in order:
        @pl.when(sends(side, step))
        def _(step=step, side=side):
            for copy in weight_copies(target(side, step), slot_of(side, step)):
                copy.start()
    for copy in weight_copies(z, z):
        copy.start()

    pl.semaphore_wait(barrier, jnp.minimum(z, 1) + jnp.minimum(last - z, 1))

    half = gkv_ref.shape[1] // 2

    def part(slot, sub):
        span = pl.ds(sub * sub_rows, sub_rows)
        acc = jnp.dot(wqb[slot, span, :], gq_ref[...], preferred_element_type=jnp.float32)
        acc += lax.dot_general(wkb[slot, span, :], gkv_ref[:, 0:half], CONTRACT_LAST, preferred_element_type=jnp.float32)
        return acc + lax.dot_general(wvb[slot, span, :], gkv_ref[:, half:], CONTRACT_LAST, preferred_element_type=jnp.float32)

    def hop(side, step, sub):
        span = pl.ds(sub * sub_rows, sub_rows)
        return pltpu.make_async_remote_copy(
            src_ref=sbuf.at[side, step, span],
            dst_ref=rbuf.at[side, step, span],
            send_sem=ssem.at[side, step, sub],
            recv_sem=rsem.at[side, step, sub],
            device_id={"ba": z - 1 if side == 0 else z + 1},
            device_id_type=MESH,
        )

    for step, side in order:
        behind = high if side == 0 else low

        @pl.when(sends(side, step))
        def _(step=step, side=side, behind=behind):
            slot = slot_of(side, step)
            for copy in weight_copies(target(side, step), slot):
                copy.wait()
            for sub in range(SUBS):
                span = pl.ds(sub * sub_rows, sub_rows)
                acc = part(slot, sub)

                @pl.when(behind)
                def _():
                    hop(side, step, sub).wait_recv()
                    sbuf[side, step, span, :] = (acc + rbuf[side, step, span, :].astype(jnp.float32)).astype(jnp.bfloat16)

                @pl.when(jnp.logical_not(behind))
                def _():
                    sbuf[side, step, span, :] = acc.astype(jnp.bfloat16)

                hop(side, step, sub).start()

    for copy in weight_copies(z, z):
        copy.wait()
    for sub in range(SUBS):
        span = pl.ds(sub * sub_rows, sub_rows)
        total_ref[span, :] = part(z, sub)
    for sub in range(SUBS):
        span = pl.ds(sub * sub_rows, sub_rows)
        for side in range(2):
            for step in range(last):
                here = (z == target(side, step)) & (high if side == 0 else low)

                @pl.when(here)
                def _(side=side, step=step):
                    hop(side, step, sub).wait_recv()
                    total_ref[span, :] += rbuf[side, step, span, :].astype(jnp.float32)

        out_ref[span, :] = total_ref[span, :].astype(jnp.bfloat16)

    for step, side in order:
        @pl.when(sends(side, step))
        def _(step=step, side=side):
            for sub in range(SUBS):
                hop(side, step, sub).wait_send()


def project_scatter(gq, gkv, w_query, w_key, w_value):
    planes = lax.axis_size("ba")
    rows = w_query.shape[0] // planes
    tokens = gq.shape[1]
    last = planes - 1
    return pl.pallas_call(
        functools.partial(scatter_kernel, planes),
        out_shape=jax.ShapeDtypeStruct((rows, tokens), jnp.bfloat16),
        in_specs=[WHOLE, WHOLE, HBM, HBM, HBM],
        out_specs=WHOLE,
        scratch_shapes=[
            pltpu.VMEM((planes, rows, w_query.shape[1]), jnp.bfloat16),
            pltpu.VMEM((planes, rows, w_key.shape[1]), jnp.bfloat16),
            pltpu.VMEM((planes, rows, w_value.shape[1]), jnp.bfloat16),
            pltpu.VMEM((2, last, rows, tokens), jnp.bfloat16),
            pltpu.VMEM((2, last, rows, tokens), jnp.bfloat16),
            pltpu.VMEM((rows, tokens), jnp.float32),
            pltpu.SemaphoreType.DMA((planes, 3)),
            pltpu.SemaphoreType.DMA((2, last, SUBS)),
            pltpu.SemaphoreType.DMA((2, last, SUBS)),
        ],
        compiler_params=pltpu.CompilerParams(
            collective_id=1, has_side_effects=True, vmem_limit_bytes=56 * 1024 * 1024
        ),
        name="project_scatter",
    )(gq, gkv, w_query, w_key, w_value)


CHUNK = 128
LOG2E = 1.4426950408889634


def attention_kernel(peers, planes, chunks, scaling, q_ref, k_ref, v_ref, seg_ref, g_ref, w_ref, gq_ref, gkv_ref,
                     wbuf, fbuf, qa, ka, va, kt, vt, segs, starts_ref, s_ref, p_ref, ot_ref, inv_ref, dvk_ref, acc_ref,
                     dsend, drecv, gqs, pair_out, pair_in, kvs,
                     local_sem, own_sem, ag_s, ag_r, x_s, x_r, d_s, d_r, gq_s, gq_r, pr_s, pr_r, kv_s, kv_r):
    me = lax.axis_index("aa")
    z = lax.axis_index("ba")
    last = planes - 1
    tok = q_ref.shape[0]
    feats = g_ref.shape[0]
    half = gkv_ref.shape[1] // 2
    barrier = pltpu.get_barrier_semaphore()

    def lanes(index):
        return pl.ds(pl.multiple_of(index * HD, HD), HD)

    def rows_of(index):
        return pl.ds(pl.multiple_of(index * tok, tok), tok)

    def peer(r):
        return lax.rem(me + r, peers)

    for r in range(1, peers):
        pl.semaphore_signal(barrier, inc=1, device_id={"aa": peer(r)}, device_id_type=MESH)
    for r in range(1, planes):
        pl.semaphore_signal(barrier, inc=1, device_id={"ba": lax.rem(z + r, planes)}, device_id_type=MESH)

    def own_copies():
        return [
            pltpu.make_async_copy(g_ref, fbuf.at[pl.ds(pl.multiple_of(z * feats, 16), feats)], own_sem.at[0]),
            pltpu.make_async_copy(q_ref.at[:, lanes(me)], qa.at[rows_of(me)], own_sem.at[1]),
            pltpu.make_async_copy(k_ref.at[:, lanes(me // 2)], ka.at[rows_of(me)], own_sem.at[2]),
            pltpu.make_async_copy(v_ref.at[:, lanes(me // 2)], va.at[rows_of(me)], own_sem.at[3]),
            pltpu.make_async_copy(seg_ref, segs.at[me], own_sem.at[4]),
        ]

    weight_copy = pltpu.make_async_copy(w_ref, wbuf, local_sem)
    for copy in own_copies():
        copy.start()
    pl.semaphore_wait(barrier, peers + planes - 2)

    def gather(side, c, s):
        source = z - s if side == 0 else z + s
        span = pl.ds(pl.multiple_of(source * feats, 16), feats)
        cols = pl.ds(c * CHUNK, CHUNK)
        return pltpu.make_async_remote_copy(
            src_ref=g_ref.at[:, cols] if s == 0 else fbuf.at[span, cols],
            dst_ref=fbuf.at[span, cols],
            send_sem=ag_s.at[side, c, s],
            recv_sem=ag_r.at[side, c, s],
            device_id={"ba": z + 1 if side == 0 else z - 1},
            device_id_type=MESH,
        )

    def arrival(side, c, s):
        source = z - 1 - s if side == 0 else z + 1 + s
        span = pl.ds(pl.multiple_of(source * feats, 16), feats)
        cols = pl.ds(c * CHUNK, CHUNK)
        return pltpu.make_async_remote_copy(
            src_ref=fbuf.at[span, cols],
            dst_ref=fbuf.at[span, cols],
            send_sem=ag_s.at[side, c, s],
            recv_sem=ag_r.at[side, c, s],
            device_id={"ba": z + 1 if side == 0 else z - 1},
            device_id_type=MESH,
        )

    def gather_sends(side, s):
        return (z >= s) & (z < last) if side == 0 else (z + s <= last) & (z > 0)

    def relay(c, s):
        for side in range(2):
            @pl.when(gather_sends(side, s))
            def _(side=side):
                if s > 0:
                    arrival(side, c, s - 1).wait_recv()
                gather(side, c, s).start()

    def finish_gather(c, steps):
        for side in range(2):
            for s in steps:
                @pl.when((z == last) if side == 0 else (z == 0))
                def _(side=side, s=s):
                    arrival(side, c, s).wait_recv()

    def exchange(kind, to, sender, peer_sem):
        shard = (q_ref.at[:, lanes(to)], k_ref.at[:, lanes(to // 2)], v_ref.at[:, lanes(to // 2)], seg_ref)[kind]
        land = (qa.at[rows_of(sender)], ka.at[rows_of(sender)], va.at[rows_of(sender)], segs.at[sender])[kind]
        return pltpu.make_async_remote_copy(
            src_ref=shard,
            dst_ref=land,
            send_sem=x_s.at[kind, peer_sem],
            recv_sem=x_r.at[kind, sender],
            device_id={"aa": to},
            device_id_type=MESH,
        )

    relay(0, 0)
    relay(1, 0)
    for r in range(1, peers):
        exchange(3, peer(r), me, r).start()
    for r in range(1, peers):
        for kind in range(3):
            exchange(kind, peer(r), me, r).start()
    weight_copy.start()
    dvk_ref[...] = jnp.zeros_like(dvk_ref)
    relay(0, 1)
    relay(1, 1)
    for copy in own_copies():
        copy.wait()
    for r in range(1, peers):
        exchange(3, me, peer(r), r).wait_recv()

    ids = segs[...]
    starts = jnp.zeros(ids.shape, jnp.float32)
    for doc in range(1, DOCS):
        before = jnp.sum(jnp.where(ids < doc, 1.0, 0.0), axis=(0, 2), keepdims=True)
        starts = jnp.where(ids == doc, before, starts)
    starts_ref[...] = starts
    relay(0, 2)
    relay(2, 0)

    def pair_rows(i, at, size):
        return pl.ds(pl.multiple_of(i * (i + 1) * tok + at, CHUNK), size)

    def stats(start, stop):
        def block(i, j):
            a = 2 * i + j

            @pl.when(a != me)
            def _():
                for kind in range(3):
                    exchange(kind, me, a, 0).wait_recv()

            kt[:, rows_of(a)] = ka[rows_of(a), :].astype(jnp.float32).T.astype(jnp.bfloat16)
            vt[:, rows_of(a)] = va[rows_of(a), :].astype(jnp.float32).T.astype(jnp.bfloat16)
            query = qa[rows_of(a), :]
            begin = starts_ref[a]

            def scores(u, diagonal):
                s = lax.dot_general(ka[rows_of(u), :], query, CONTRACT_LAST, preferred_element_type=jnp.float32)
                key = lax.broadcasted_iota(jnp.int32, (tok, tok), 0)
                allowed = (key + u * tok).astype(jnp.float32) >= begin
                if diagonal:
                    allowed &= key <= lax.broadcasted_iota(jnp.int32, (tok, tok), 1)
                s = jnp.where(allowed, s * (scaling * LOG2E), NEG_FILL)
                s_ref[rows_of(u), :] = s
                return fold_rows(s, jnp.max)

            top = lax.fori_loop(0, a, lambda u, t: jnp.maximum(t, scores(u, False)),
                                jnp.full((8, tok), NEG_FILL, jnp.float32))
            top = jnp.max(jnp.maximum(top, scores(a, True)), axis=0, keepdims=True)

            def weights(u, state):
                total, out = state
                p = jnp.exp2(s_ref[rows_of(u), :] - top)
                low = p.astype(jnp.bfloat16)
                for c in range(chunks):
                    p_ref[c, pair_rows(i, u * tok, tok), j * CHUNK : (j + 1) * CHUNK] = low[:, c * CHUNK : (c + 1) * CHUNK]
                return (total + fold_rows(p, jnp.sum),
                        out + jnp.dot(vt[:, rows_of(u)], low, preferred_element_type=jnp.float32))

            state = (jnp.zeros((8, tok), jnp.float32), jnp.zeros((HD, tok), jnp.float32))
            total, out = lax.fori_loop(0, a + 1, weights, state)
            inverse = 1.0 / jnp.sum(total, axis=0, keepdims=True)
            inv_ref[a] = inverse
            ot_ref[a] = out * inverse
            if j == 0:
                for c in range(chunks):
                    p_ref[c, pair_rows(i, (a + 1) * tok, tok), 0:CHUNK] = jnp.zeros((tok, CHUNK), jnp.bfloat16)

        def pair(i, carry):
            block(i, 0)
            block(i, 1)
            return carry

        lax.fori_loop(start, stop, pair, 0)

    def dout_send(c, to):
        return pltpu.make_async_remote_copy(
            src_ref=dsend.at[c, to],
            dst_ref=drecv.at[c, me],
            send_sem=d_s.at[c, to],
            recv_sem=d_r.at[c, me],
            device_id={"aa": to},
            device_id_type=MESH,
        )

    def dout_arrival(c, sender):
        return pltpu.make_async_remote_copy(
            src_ref=dsend.at[c, sender],
            dst_ref=drecv.at[c, sender],
            send_sem=d_s.at[c, sender],
            recv_sem=d_r.at[c, sender],
            device_id={"aa": sender},
            device_id_type=MESH,
        )

    depth = planes // 2 * feats
    near = z // (planes // 2)

    def project_half(c, which):
        side = near if which == 0 else 1 - near
        span = pl.ds(pl.multiple_of(side * depth, CHUNK), depth)
        finish_gather(c, range(1) if which == 0 else range(1, last))
        group = peers // 2

        def heads(i, carry):
            rows = pl.ds(pl.multiple_of(i * (group * HD), HD), group * HD)
            out = jnp.dot(wbuf[rows, span], fbuf[span, c * CHUNK : (c + 1) * CHUNK], preferred_element_type=jnp.float32)
            if which == 0:
                acc_ref[c, rows, :] = out
                return carry
            out += acc_ref[c, rows, :]
            for j in range(group):
                to = i * group + j
                dsend[c, to] = out[j * HD : (j + 1) * HD, :].astype(jnp.bfloat16)

                @pl.when(to != me)
                def _():
                    dout_send(c, to).start()

            return carry

        lax.fori_loop(0, peers // group, heads, 0)
        if which == 1:
            drecv[c, me] = dsend[c, me]

    def gq_copy(c, to):
        return pltpu.make_async_remote_copy(
            src_ref=gqs.at[c, to],
            dst_ref=gq_ref.at[lanes(me), pl.ds(c * CHUNK, CHUNK)],
            send_sem=gq_s.at[c, to],
            recv_sem=gq_r.at[c, me],
            device_id={"aa": to},
            device_id_type=MESH,
        )

    def gq_arrival(c, sender):
        return pltpu.make_async_remote_copy(
            src_ref=gqs.at[c, sender],
            dst_ref=gq_ref.at[lanes(sender), pl.ds(c * CHUNK, CHUNK)],
            send_sem=gq_s.at[c, sender],
            recv_sem=gq_r.at[c, sender],
            device_id={"aa": sender},
            device_id_type=MESH,
        )

    def gq_local(c):
        return pltpu.make_async_copy(gqs.at[c, me], gq_ref.at[lanes(me), pl.ds(c * CHUNK, CHUNK)], own_sem.at[c])

    odd = lax.rem(me, 2)
    partner = me + 1 - 2 * odd

    def pair_span(i):
        return pl.ds(pl.multiple_of(i * (2 * tok), CHUNK), 2 * tok)

    def pair_copy(i):
        return pltpu.make_async_remote_copy(
            src_ref=pair_out.at[pair_span(i)],
            dst_ref=pair_in.at[pair_span(i)],
            send_sem=pr_s.at[i],
            recv_sem=pr_r.at[i],
            device_id={"aa": partner},
            device_id_type=MESH,
        )

    def grads(c):
        final = c == chunks - 1

        def pair(step, carry):
            i = peers // 2 - 1 - step
            douts, queries, deltas = [], [], []
            for j in range(2):
                a = 2 * i + j

                @pl.when(a != me)
                def _():
                    dout_arrival(c, a).wait_recv()

                cols = slice(c * CHUNK, (c + 1) * CHUNK)
                dout = (drecv[c, a].astype(jnp.float32) * inv_ref[a, :, cols]).astype(jnp.bfloat16).astype(jnp.float32)
                deltas.append(jnp.sum(dout * ot_ref[a, :, cols], axis=0, keepdims=True))
                douts.append(dout)
                queries.append(qa[pl.ds(pl.multiple_of(a * tok + c * CHUNK, CHUNK), CHUNK), :])
            dout = jnp.concatenate(douts, axis=1)
            dout_low = dout.astype(jnp.bfloat16)
            dout_rows = dout.T.astype(jnp.bfloat16)
            delta = jnp.concatenate(deltas, axis=1)
            query = jnp.concatenate(queries, axis=0)

            def unit(u, grad_q):
                span = pair_span(u)
                p = p_ref[c, pair_rows(i, u * (2 * tok), 2 * tok), :]
                dp = jnp.dot(va[span, :], dout_low, preferred_element_type=jnp.float32)
                ds = (p.astype(jnp.float32) * (dp - delta)).astype(jnp.bfloat16)
                dvk_ref[span, 0:HD] += jnp.dot(p, dout_rows, preferred_element_type=jnp.float32)
                dvk_ref[span, HD:] += jnp.dot(ds, query, preferred_element_type=jnp.float32)
                return grad_q + jnp.dot(kt[:, span], ds, preferred_element_type=jnp.float32)

            grad_q = lax.fori_loop(0, i + 1, unit, jnp.zeros((HD, 2 * CHUNK), jnp.float32))
            for j in range(2):
                a = 2 * i + j
                gqs[c, a] = (grad_q[:, j * CHUNK : (j + 1) * CHUNK] * scaling).astype(jnp.bfloat16)

                @pl.when(a != me)
                def _():
                    gq_copy(c, a).start()

            if final:
                span = pair_span(i)

                @pl.when(odd == 0)
                def _():
                    pair_out[span, :] = dvk_ref[span, 0:HD].astype(jnp.bfloat16)

                @pl.when(odd == 1)
                def _():
                    pair_out[span, :] = (dvk_ref[span, HD:] * scaling).astype(jnp.bfloat16)

                pair_copy(i).start()

            return carry

        lax.fori_loop(0, peers // 2, pair, 0)
        gq_local(c).start()

    stats(0, 3)
    relay(1, 2)
    stats(3, peers // 2)
    relay(2, 1)
    weight_copy.wait()
    project_half(0, 0)
    project_half(0, 1)
    relay(2, 2)
    project_half(1, 0)
    project_half(2, 0)
    project_half(1, 1)
    grads(0)
    grads(1)
    project_half(2, 1)
    grads(2)

    def join(step, carry):
        i = peers // 2 - 1 - step
        span = pair_span(i)
        pair_copy(i).wait_recv()

        @pl.when(odd == 0)
        def _():
            kvs[span, :] = (dvk_ref[span, HD:] * scaling + pair_in[span, :].astype(jnp.float32)).astype(jnp.bfloat16)

        @pl.when(odd == 1)
        def _():
            kvs[span, :] = (dvk_ref[span, 0:HD] + pair_in[span, :].astype(jnp.float32)).astype(jnp.bfloat16)

        return carry

    lax.fori_loop(0, peers // 2, join, 0)

    def kv_cols(sender):
        return pl.ds(pl.multiple_of(lax.rem(sender, 2) * half + sender // 2 * HD, HD), HD)

    def kv_copy(to):
        return pltpu.make_async_remote_copy(
            src_ref=kvs.at[rows_of(to)],
            dst_ref=gkv_ref.at[:, kv_cols(me)],
            send_sem=kv_s.at[to],
            recv_sem=kv_r.at[me],
            device_id={"aa": to},
            device_id_type=MESH,
        )

    def kv_arrival(sender):
        return pltpu.make_async_remote_copy(
            src_ref=kvs.at[rows_of(sender)],
            dst_ref=gkv_ref.at[:, kv_cols(sender)],
            send_sem=kv_s.at[sender],
            recv_sem=kv_r.at[sender],
            device_id={"aa": sender},
            device_id_type=MESH,
        )

    for r in range(1, peers):
        kv_copy(peer(r)).start()
    kv_local = pltpu.make_async_copy(kvs.at[rows_of(me)], gkv_ref.at[:, kv_cols(me)], own_sem.at[3])
    kv_local.start()

    for c in range(chunks):
        gq_local(c).wait()
    kv_local.wait()
    for r in range(1, peers):
        other = peer(r)
        for c in range(chunks):
            gq_arrival(c, other).wait_recv()
        kv_arrival(other).wait_recv()
    for r in range(1, peers):
        other = peer(r)
        for kind in range(4):
            exchange(kind, other, me, r).wait_send()
        for c in range(chunks):
            dout_send(c, other).wait_send()
            gq_copy(c, other).wait_send()
        kv_copy(other).wait_send()
    for i in range(peers // 2):
        pair_copy(i).wait_send()
    for side in range(2):
        for s in range(last):
            @pl.when(gather_sends(side, s))
            def _(side=side, s=s):
                for c in range(chunks):
                    gather(side, c, s).wait_send()


def attention_grads(query, keys, values, segment_ids, grad_out, w_out, scaling):
    peers, planes = lax.axis_size("aa"), lax.axis_size("ba")
    tok = query.shape[0]
    chunks = tok // CHUNK
    total = peers * tok
    pairs = peers // 2
    low, full = jnp.bfloat16, jnp.float32
    return pl.pallas_call(
        functools.partial(attention_kernel, peers, planes, chunks, scaling),
        out_shape=[
            jax.ShapeDtypeStruct((query.shape[1], tok), low),
            jax.ShapeDtypeStruct((tok, 2 * keys.shape[1]), low),
        ],
        in_specs=[HBM] * 6,
        out_specs=[WHOLE, WHOLE],
        scratch_shapes=[
            pltpu.VMEM(w_out.shape, low),
            pltpu.VMEM((w_out.shape[1], tok), low),
            pltpu.VMEM((total, HD), low),
            pltpu.VMEM((total, HD), low),
            pltpu.VMEM((total, HD), low),
            pltpu.VMEM((HD, total), low),
            pltpu.VMEM((HD, total), low),
            pltpu.VMEM((peers, 1, tok), jnp.int32),
            pltpu.VMEM((peers, 1, tok), full),
            pltpu.VMEM((total, tok), full),
            pltpu.VMEM((chunks, pairs * (pairs + 1) * tok, 2 * CHUNK), low),
            pltpu.VMEM((peers, HD, tok), full),
            pltpu.VMEM((peers, 1, tok), full),
            pltpu.VMEM((total, 2 * HD), full),
            pltpu.VMEM((chunks, peers * HD, CHUNK), full),
            pltpu.VMEM((chunks, peers, HD, CHUNK), low),
            pltpu.VMEM((chunks, peers, HD, CHUNK), low),
            pltpu.VMEM((chunks, peers, HD, CHUNK), low),
            pltpu.VMEM((total, HD), low),
            pltpu.VMEM((total, HD), low),
            pltpu.VMEM((total, HD), low),
            pltpu.SemaphoreType.DMA,
            pltpu.SemaphoreType.DMA((5,)),
            pltpu.SemaphoreType.DMA((2, chunks, planes - 1)),
            pltpu.SemaphoreType.DMA((2, chunks, planes - 1)),
            pltpu.SemaphoreType.DMA((4, peers)),
            pltpu.SemaphoreType.DMA((4, peers)),
            pltpu.SemaphoreType.DMA((chunks, peers)),
            pltpu.SemaphoreType.DMA((chunks, peers)),
            pltpu.SemaphoreType.DMA((chunks, peers)),
            pltpu.SemaphoreType.DMA((chunks, peers)),
            pltpu.SemaphoreType.DMA((pairs,)),
            pltpu.SemaphoreType.DMA((pairs,)),
            pltpu.SemaphoreType.DMA((peers,)),
            pltpu.SemaphoreType.DMA((peers,)),
        ],
        compiler_params=pltpu.CompilerParams(
            collective_id=0, has_side_effects=True, vmem_limit_bytes=60 * 1024 * 1024
        ),
        name="attention_grads",
    )(query, keys, values, segment_ids.reshape(1, -1), grad_out.T, w_out)


def local(query, keys, values, grad_out, segment_ids, w_query, w_key, w_value, w_out):
    seq_devices, planes = lax.axis_size("aa"), lax.axis_size("ba")
    heads, groups = query.shape[1] // HD, keys.shape[1] // HD
    fits = heads == seq_devices and 2 * groups == heads and planes == 4 and query.shape[0] == 3 * CHUNK
    if not fits:
        return local_ring(query, keys, values, grad_out, segment_ids, w_query, w_key, w_value, w_out)
    scaling = (D / HQ) ** (-0.5)
    grad_q, grad_kv = attention_grads(query, keys, values, segment_ids, grad_out, w_out, scaling)
    return project_scatter(grad_q, grad_kv, w_query, w_key, w_value).T


def solution(mesh):
    return jax.shard_map(
        local,
        mesh=mesh,
        in_specs=(
            P("aa", "ba"),
            P("aa", "ba"),
            P("aa", "ba"),
            P("aa", "ba"),
            P("aa"),
            P(None, "ba"),
            P(None, "ba"),
            P(None, "ba"),
            P("ba", None),
        ),
        out_specs=P("aa", "ba"),
        check_vma=False,
    )
```

```python
import functools

import jax
import jax.numpy as jnp
from jax import lax
from jax.experimental import pallas as pl
from jax.experimental.pallas import tpu as pltpu
from jax.sharding import PartitionSpec as P

D = 5376
HQ = 32
HD = 128
DOCS = 6


NEG_FILL = -1e30


def from_behind(value, axis, steps):
    count = lax.axis_size(axis)
    pairs = [(source, (source + steps) % count) for source in range(count)]
    return lax.ppermute(value, axis, pairs)


def block_scores(query, dout, keys, values, query_pos, query_seg, key_pos, key_seg, scaling):
    row_count = query.shape[0]
    col_count = keys.shape[0]
    groups = keys.shape[1] // HD
    query_four = query.reshape(row_count, groups, 2, HD)
    dout_four = dout.reshape(row_count, groups, 2, HD)
    key_three = keys.reshape(col_count, groups, HD)
    value_three = values.reshape(col_count, groups, HD)
    scores = (
        jnp.einsum("iagd,jad->agij", query_four, key_three, preferred_element_type=jnp.float32)
        * scaling
    )
    dprobs = jnp.einsum(
        "iagd,jad->agij", dout_four, value_three, preferred_element_type=jnp.float32
    )
    allowed = (key_pos[None, :] <= query_pos[:, None]) & (key_seg[None, :] == query_seg[:, None])
    return (scores, dprobs, allowed, query_four, dout_four, key_three)


def forward_stats(
    query, dout, keys, values, query_pos, query_seg, key_pos, key_seg, scaling, state
):
    run_max, run_sum, run_dot = state
    scores, dprobs, allowed, unused_q, unused_d, unused_k = block_scores(
        query, dout, keys, values, query_pos, query_seg, key_pos, key_seg, scaling
    )
    masked = jnp.where(allowed, scores, NEG_FILL)
    new_max = jnp.maximum(run_max, jnp.max(masked, axis=-1))
    expo = jnp.where(allowed, jnp.exp(scores - new_max[..., None]), 0.0)
    return (new_max, jnp.sum(expo, axis=-1), jnp.sum(expo * dprobs, axis=-1))


def block_grads(
    query, dout, row_lse, row_delta, keys, values, query_pos, query_seg, key_pos, key_seg, scaling
):
    scores, dprobs, allowed, query_four, dout_four, key_three = block_scores(
        query, dout, keys, values, query_pos, query_seg, key_pos, key_seg, scaling
    )
    softmax_w = jnp.where(allowed, jnp.exp(scores - row_lse[..., None]), 0.0)
    dscores = softmax_w * (dprobs - row_delta[..., None])
    softmax_low = softmax_w.astype(jnp.bfloat16)
    dscores_low = dscores.astype(jnp.bfloat16)
    grad_v = jnp.einsum(
        "agij,iagd->jad", softmax_low, dout_four, preferred_element_type=jnp.float32
    )
    grad_k = (
        jnp.einsum("agij,iagd->jad", dscores_low, query_four, preferred_element_type=jnp.float32)
        * scaling
    )
    grad_q = (
        jnp.einsum("agij,jad->iagd", dscores_low, key_three, preferred_element_type=jnp.float32)
        * scaling
    )
    return (
        grad_q.reshape(query.shape[0], -1),
        grad_k.reshape(keys.shape[0], -1),
        grad_v.reshape(keys.shape[0], -1),
    )


def project_back(grad, weight):
    return lax.dot_general(
        grad, weight, (((1,), (1,)), ((), ())), preferred_element_type=jnp.float32
    )


def local_ring(query, keys, values, grad_out, segment_ids, w_query, w_key, w_value, w_out):
    seq_devices = lax.axis_size("aa")
    own_index = lax.axis_index("aa")
    tok_count = query.shape[0]
    scaling = (D / HQ) ** (-0.5)
    groups = keys.shape[1] // HD
    all_seg = lax.all_gather(segment_ids, "aa", axis=0, tiled=True)
    dout = project_back(lax.all_gather(grad_out, "ba", axis=1, tiled=True), w_out).astype(
        jnp.bfloat16
    )
    offsets = lax.iota(jnp.int32, tok_count)
    own_pos = own_index * tok_count + offsets
    own_seg = lax.dynamic_slice_in_dim(all_seg, own_index * tok_count, tok_count)
    stat_shape = (groups, 2, tok_count)
    stats_start = (
        jnp.full(stat_shape, NEG_FILL, jnp.float32),
        jnp.zeros(stat_shape, jnp.float32),
        jnp.zeros(stat_shape, jnp.float32),
    )
    piece = (
        lax.all_gather(keys, "aa", axis=0, tiled=True),
        lax.all_gather(values, "aa", axis=0, tiled=True),
    )
    width = piece[0].shape[0]
    key_pos = lax.iota(jnp.int32, width)
    key_seg = all_seg
    run_max, run_sum, run_dot = forward_stats(
        query, dout, piece[0], piece[1], own_pos, own_seg, key_pos, key_seg, scaling, stats_start
    )
    row_lse = run_max + jnp.log(run_sum)
    row_delta = run_dot / run_sum
    zero_q = jnp.zeros(query.shape, jnp.float32)
    zero_k = jnp.zeros(keys.shape, jnp.float32)

    def step_keys(step_index, state):
        (keys_now, values_now), (dk_now, dv_now), grad_q = state
        anchor = (own_index - step_index) % seq_devices
        key_pos = anchor * tok_count + offsets
        key_seg = lax.dynamic_slice_in_dim(all_seg, anchor * tok_count, tok_count)
        add_q, add_k, add_v = block_grads(
            query,
            dout,
            row_lse,
            row_delta,
            keys_now,
            values_now,
            own_pos,
            own_seg,
            key_pos,
            key_seg,
            scaling,
        )
        bundle_next = from_behind((keys_now, values_now), "aa", 1)
        sums_next = (
            from_behind((dk_now + add_k).astype(jnp.bfloat16), "aa", 1).astype(jnp.float32),
            from_behind((dv_now + add_v).astype(jnp.bfloat16), "aa", 1).astype(jnp.float32),
        )
        return (bundle_next, sums_next, grad_q + add_q)

    initial = ((keys, values), (zero_k, zero_k), zero_q)
    final = lax.fori_loop(0, seq_devices, step_keys, initial)
    grad_q = final[2]
    grad_k = final[1][0]
    grad_v = final[1][1]
    partial_value = (
        project_back(grad_q.astype(jnp.bfloat16), w_query)
        + project_back(grad_k.astype(jnp.bfloat16), w_key)
        + project_back(grad_v.astype(jnp.bfloat16), w_value)
    )
    return lax.psum_scatter(
        partial_value.astype(jnp.bfloat16), "ba", scatter_dimension=1, tiled=True
    )


def fold_rows(value, op):
    return op(value.reshape(-1, 8, value.shape[1]), axis=0)


CONTRACT_LAST = (((1,), (1,)), ((), ()))


WHOLE = pl.BlockSpec(memory_space=pltpu.VMEM)


MESH = pl.DeviceIdType.MESH
HBM = pl.BlockSpec(memory_space=pl.ANY)
SUBS = 3


def scatter_kernel(planes, gq_ref, gkv_ref, wq_ref, wk_ref, wv_ref, out_ref, wqb, wkb, wvb, sbuf, rbuf, total_ref, wsem, ssem, rsem):
    z = lax.axis_index("ba")
    barrier = pltpu.get_barrier_semaphore()
    last = planes - 1
    low = z > 0
    high = z < last

    @pl.when(low)
    def _():
        pl.semaphore_signal(barrier, inc=1, device_id={"ba": z - 1}, device_id_type=MESH)

    @pl.when(high)
    def _():
        pl.semaphore_signal(barrier, inc=1, device_id={"ba": z + 1}, device_id_type=MESH)

    rows = out_ref.shape[0]
    sub_rows = rows // SUBS

    def target(side, step):
        return jnp.where(side == 0, step, last - step)

    near = jnp.where(2 * z > last, 0, 1)
    sides = (near, 1 - near)
    counts = (jnp.maximum(z, last - z), jnp.minimum(z, last - z))

    def weight_copies(feature):
        span = pl.ds(pl.multiple_of(feature * rows, 16), rows)
        return [
            pltpu.make_async_copy(src.at[span], dst.at[feature], wsem.at[feature, part])
            for part, (src, dst) in enumerate(((wq_ref, wqb), (wk_ref, wkb), (wv_ref, wvb)))
        ]

    for step in range(last):
        for which in range(2):
            @pl.when(step < counts[which])
            def _(step=step, which=which):
                for copy in weight_copies(target(sides[which], step)):
                    copy.start()
    for copy in weight_copies(z):
        copy.start()

    pl.semaphore_wait(barrier, jnp.minimum(z, 1) + jnp.minimum(last - z, 1))

    half = gkv_ref.shape[1] // 2

    def part(slot, sub):
        span = pl.ds(sub * sub_rows, sub_rows)
        acc = jnp.dot(wqb[slot, span, :], gq_ref[...], preferred_element_type=jnp.float32)
        acc += lax.dot_general(wkb[slot, span, :], gkv_ref[:, 0:half], CONTRACT_LAST, preferred_element_type=jnp.float32)
        return acc + lax.dot_general(wvb[slot, span, :], gkv_ref[:, half:], CONTRACT_LAST, preferred_element_type=jnp.float32)

    def hop(side, step, sub):
        span = pl.ds(sub * sub_rows, sub_rows)
        return pltpu.make_async_remote_copy(
            src_ref=sbuf.at[side, step, span],
            dst_ref=rbuf.at[side, step, span],
            send_sem=ssem.at[side, step, sub],
            recv_sem=rsem.at[side, step, sub],
            device_id={"ba": jnp.where(side == 0, z - 1, z + 1)},
            device_id_type=MESH,
        )

    inner = low & high
    order = sorted(
        [(step * SUBS + sub + 2 * which * (step + 1) - 0.5 * which, which, step, sub)
         for which in range(2) for step in range(last - which) for sub in range(SUBS)]
    )
    for _unused, which, step, sub in order:
        @pl.when(step < counts[which])
        def _(which=which, step=step, sub=sub):
            side = sides[which]
            feature = target(side, step)
            if sub == 0:
                for copy in weight_copies(feature):
                    copy.wait()
            span = pl.ds(sub * sub_rows, sub_rows)
            acc = part(feature, sub)

            @pl.when(inner)
            def _():
                hop(side, step, sub).wait_recv()
                sbuf[side, step, span, :] = (acc + rbuf[side, step, span, :].astype(jnp.float32)).astype(jnp.bfloat16)

            @pl.when(jnp.logical_not(inner))
            def _():
                sbuf[side, step, span, :] = acc.astype(jnp.bfloat16)

            hop(side, step, sub).start()

    for copy in weight_copies(z):
        copy.wait()
    for sub in range(SUBS):
        span = pl.ds(sub * sub_rows, sub_rows)
        total_ref[span, :] = part(z, sub)
    for sub in range(SUBS):
        span = pl.ds(sub * sub_rows, sub_rows)
        for side in range(2):
            for step in range(last):
                here = (z == target(side, step)) & (high if side == 0 else low)

                @pl.when(here)
                def _(side=side, step=step):
                    hop(side, step, sub).wait_recv()
                    total_ref[span, :] += rbuf[side, step, span, :].astype(jnp.float32)

        out_ref[span, :] = total_ref[span, :].astype(jnp.bfloat16)

    for which in range(2):
        for step in range(last):
            @pl.when(step < counts[which])
            def _(which=which, step=step):
                for sub in range(SUBS):
                    hop(sides[which], step, sub).wait_send()


def project_scatter(gq, gkv, w_query, w_key, w_value):
    planes = lax.axis_size("ba")
    rows = w_query.shape[0] // planes
    tokens = gq.shape[1]
    last = planes - 1
    return pl.pallas_call(
        functools.partial(scatter_kernel, planes),
        out_shape=jax.ShapeDtypeStruct((rows, tokens), jnp.bfloat16),
        in_specs=[WHOLE, WHOLE, HBM, HBM, HBM],
        out_specs=WHOLE,
        scratch_shapes=[
            pltpu.VMEM((planes, rows, w_query.shape[1]), jnp.bfloat16),
            pltpu.VMEM((planes, rows, w_key.shape[1]), jnp.bfloat16),
            pltpu.VMEM((planes, rows, w_value.shape[1]), jnp.bfloat16),
            pltpu.VMEM((2, last, rows, tokens), jnp.bfloat16),
            pltpu.VMEM((2, last, rows, tokens), jnp.bfloat16),
            pltpu.VMEM((rows, tokens), jnp.float32),
            pltpu.SemaphoreType.DMA((planes, 3)),
            pltpu.SemaphoreType.DMA((2, last, SUBS)),
            pltpu.SemaphoreType.DMA((2, last, SUBS)),
        ],
        compiler_params=pltpu.CompilerParams(
            collective_id=1, has_side_effects=True, vmem_limit_bytes=56 * 1024 * 1024
        ),
        name="project_scatter",
    )(gq, gkv, w_query, w_key, w_value)


CHUNK = 128
LOG2E = 1.4426950408889634


def attention_kernel(peers, planes, chunks, scaling, q_ref, k_ref, v_ref, seg_ref, g_ref, w_ref, gq_ref, gkv_ref,
                     wbuf, fbuf, qa, ka, va, kt, vt, segs, starts_ref, s_ref, p_ref, ot_ref, inv_ref, dvk_ref, acc_ref,
                     dsend, drecv, gqs, pair_out, pair_in, kvs,
                     local_sem, own_sem, f_s, ag_s, ag_r, x_s, x_r, d_s, d_r, gq_s, gq_r, pr_s, pr_r, kv_s, kv_r):
    me = lax.axis_index("aa")
    z = lax.axis_index("ba")
    last = planes - 1
    tok = q_ref.shape[0]
    feats = g_ref.shape[0]
    half = gkv_ref.shape[1] // 2
    barrier = pltpu.get_barrier_semaphore()

    def lanes(index):
        return pl.ds(pl.multiple_of(index * HD, HD), HD)

    def rows_of(index):
        return pl.ds(pl.multiple_of(index * tok, tok), tok)

    def peer(r):
        return lax.rem(me + r, peers)

    for r in range(1, peers):
        pl.semaphore_signal(barrier, inc=1, device_id={"aa": peer(r)}, device_id_type=MESH)
    for r in range(1, planes):
        pl.semaphore_signal(barrier, inc=1, device_id={"ba": lax.rem(z + r, planes)}, device_id_type=MESH)

    def own_copies():
        return [
            pltpu.make_async_copy(g_ref, fbuf.at[pl.ds(pl.multiple_of(z * feats, 16), feats)], own_sem.at[0]),
            pltpu.make_async_copy(q_ref.at[:, lanes(me)], qa.at[rows_of(me)], own_sem.at[1]),
            pltpu.make_async_copy(k_ref.at[:, lanes(me // 2)], ka.at[rows_of(me)], own_sem.at[2]),
            pltpu.make_async_copy(v_ref.at[:, lanes(me // 2)], va.at[rows_of(me)], own_sem.at[3]),
            pltpu.make_async_copy(seg_ref, segs.at[me], own_sem.at[4]),
        ]

    weight_copy = pltpu.make_async_copy(w_ref, wbuf, local_sem)
    for copy in own_copies():
        copy.start()
    pl.semaphore_wait(barrier, peers + planes - 2)

    def gather(side, c, s):
        source = z - s if side == 0 else z + s
        span = pl.ds(pl.multiple_of(source * feats, 16), feats)
        cols = pl.ds(c * CHUNK, CHUNK)
        return pltpu.make_async_remote_copy(
            src_ref=g_ref.at[:, cols] if s == 0 else fbuf.at[span, cols],
            dst_ref=fbuf.at[span, cols],
            send_sem=ag_s.at[side, c, s],
            recv_sem=ag_r.at[side, c, s],
            device_id={"ba": z + 1 if side == 0 else z - 1},
            device_id_type=MESH,
        )

    def arrival(side, c, s):
        source = z - 1 - s if side == 0 else z + 1 + s
        span = pl.ds(pl.multiple_of(source * feats, 16), feats)
        cols = pl.ds(c * CHUNK, CHUNK)
        return pltpu.make_async_remote_copy(
            src_ref=fbuf.at[span, cols],
            dst_ref=fbuf.at[span, cols],
            send_sem=ag_s.at[side, c, s],
            recv_sem=ag_r.at[side, c, s],
            device_id={"ba": z + 1 if side == 0 else z - 1},
            device_id_type=MESH,
        )

    def gather_sends(side, s):
        return (z >= s) & (z < last) if side == 0 else (z + s <= last) & (z > 0)

    def relay(c, s):
        for side in range(2):
            @pl.when(gather_sends(side, s))
            def _(side=side):
                if s > 0:
                    arrival(side, c, s - 1).wait_recv()
                gather(side, c, s).start()

    def finish_gather(c, steps):
        for side in range(2):
            for s in steps:
                @pl.when((z == last) if side == 0 else (z == 0))
                def _(side=side, s=s):
                    arrival(side, c, s).wait_recv()

    odd = lax.rem(me, 2)
    partner = me + 1 - 2 * odd

    def forward(kind, sender, r):
        land = (ka if kind == 1 else va).at[rows_of(sender)]
        return pltpu.make_async_remote_copy(
            src_ref=land,
            dst_ref=land,
            send_sem=f_s.at[kind - 1, r],
            recv_sem=x_r.at[kind, sender],
            device_id={"aa": partner},
            device_id_type=MESH,
        )

    def exchange(kind, to, sender, peer_sem):
        shard = (q_ref.at[:, lanes(to)], k_ref.at[:, lanes(to // 2)], v_ref.at[:, lanes(to // 2)], seg_ref)[kind]
        land = (qa.at[rows_of(sender)], ka.at[rows_of(sender)], va.at[rows_of(sender)], segs.at[sender])[kind]
        return pltpu.make_async_remote_copy(
            src_ref=shard,
            dst_ref=land,
            send_sem=x_s.at[kind, peer_sem],
            recv_sem=x_r.at[kind, sender],
            device_id={"aa": to},
            device_id_type=MESH,
        )

    relay(0, 0)
    relay(1, 0)
    for r in range(1, peers):
        exchange(3, peer(r), me, r).start()
    for r in range(1, peers):
        exchange(0, peer(r), me, r).start()
    for kind in (1, 2):
        exchange(kind, partner, me, 1).start()
        for r in range(2, peers, 2):
            exchange(kind, peer(r), me, r).start()
    weight_copy.start()
    dvk_ref[...] = jnp.zeros_like(dvk_ref)
    relay(0, 1)
    relay(1, 1)
    for copy in own_copies():
        copy.wait()
    for r in range(1, peers):
        exchange(3, me, peer(r), r).wait_recv()

    ids = segs[...]
    starts = jnp.zeros(ids.shape, jnp.float32)
    for doc in range(1, DOCS):
        before = jnp.sum(jnp.where(ids < doc, 1.0, 0.0), axis=(0, 2), keepdims=True)
        starts = jnp.where(ids == doc, before, starts)
    starts_ref[...] = starts
    for kind in (1, 2):
        for r in range(2, peers, 2):
            exchange(kind, me, peer(r), r).wait_recv()
            forward(kind, peer(r), r).start()

    def pair_rows(i, at, size):
        return pl.ds(pl.multiple_of(i * (i + 1) * tok + at, CHUNK), size)

    def stats(start, stop):
        def block(i, j):
            a = 2 * i + j

            @pl.when(a != me)
            def _():
                exchange(0, me, a, 0).wait_recv()

            @pl.when(lax.rem(a + me, 2) == 1)
            def _():
                for kind in (1, 2):
                    exchange(kind, me, a, 0).wait_recv()

            kt[:, rows_of(a)] = ka[rows_of(a), :].astype(jnp.float32).T.astype(jnp.bfloat16)
            vt[:, rows_of(a)] = va[rows_of(a), :].astype(jnp.float32).T.astype(jnp.bfloat16)
            query = qa[rows_of(a), :]
            begin = starts_ref[a]

            def scores(u, diagonal):
                s = lax.dot_general(ka[rows_of(u), :], query, CONTRACT_LAST, preferred_element_type=jnp.float32)
                key = lax.broadcasted_iota(jnp.int32, (tok, tok), 0)
                allowed = (key + u * tok).astype(jnp.float32) >= begin
                if diagonal:
                    allowed &= key <= lax.broadcasted_iota(jnp.int32, (tok, tok), 1)
                s = jnp.where(allowed, s * (scaling * LOG2E), NEG_FILL)
                s_ref[rows_of(u), :] = s
                return fold_rows(s, jnp.max)

            top = lax.fori_loop(0, a, lambda u, t: jnp.maximum(t, scores(u, False)),
                                jnp.full((8, tok), NEG_FILL, jnp.float32))
            top = jnp.max(jnp.maximum(top, scores(a, True)), axis=0, keepdims=True)

            def weights(u, state):
                total, out = state
                p = jnp.exp2(s_ref[rows_of(u), :] - top)
                low = p.astype(jnp.bfloat16)
                for c in range(chunks):
                    p_ref[c, pair_rows(i, u * tok, tok), j * CHUNK : (j + 1) * CHUNK] = low[:, c * CHUNK : (c + 1) * CHUNK]
                return (total + fold_rows(p, jnp.sum),
                        out + jnp.dot(vt[:, rows_of(u)], low, preferred_element_type=jnp.float32))

            state = (jnp.zeros((8, tok), jnp.float32), jnp.zeros((HD, tok), jnp.float32))
            total, out = lax.fori_loop(0, a + 1, weights, state)
            inverse = 1.0 / jnp.sum(total, axis=0, keepdims=True)
            inv_ref[a] = inverse
            ot_ref[a] = out * inverse
            if j == 0:
                for c in range(chunks):
                    p_ref[c, pair_rows(i, (a + 1) * tok, tok), 0:CHUNK] = jnp.zeros((tok, CHUNK), jnp.bfloat16)

        def pair(i, carry):
            block(i, 0)
            block(i, 1)
            return carry

        lax.fori_loop(start, stop, pair, 0)

    def dout_send(c, to):
        return pltpu.make_async_remote_copy(
            src_ref=dsend.at[c, to],
            dst_ref=drecv.at[c, me],
            send_sem=d_s.at[c, to],
            recv_sem=d_r.at[c, me],
            device_id={"aa": to},
            device_id_type=MESH,
        )

    def dout_arrival(c, sender):
        return pltpu.make_async_remote_copy(
            src_ref=dsend.at[c, sender],
            dst_ref=drecv.at[c, sender],
            send_sem=d_s.at[c, sender],
            recv_sem=d_r.at[c, sender],
            device_id={"aa": sender},
            device_id_type=MESH,
        )

    depth = planes // 2 * feats
    near = z // (planes // 2)

    def project_half(c, which):
        side = near if which == 0 else 1 - near
        span = pl.ds(pl.multiple_of(side * depth, CHUNK), depth)
        finish_gather(c, range(1) if which == 0 else range(1, last))
        group = peers // 2

        def heads(i, carry):
            rows = pl.ds(pl.multiple_of(i * (group * HD), HD), group * HD)
            out = jnp.dot(wbuf[rows, span], fbuf[span, c * CHUNK : (c + 1) * CHUNK], preferred_element_type=jnp.float32)
            if which == 0:
                acc_ref[c, rows, :] = out
                return carry
            out += acc_ref[c, rows, :]
            for j in range(group):
                to = i * group + j
                dsend[c, to] = out[j * HD : (j + 1) * HD, :].astype(jnp.bfloat16)

                @pl.when(to != me)
                def _():
                    dout_send(c, to).start()

            return carry

        lax.fori_loop(0, peers // group, heads, 0)
        if which == 1:
            drecv[c, me] = dsend[c, me]

    def gq_copy(c, to):
        return pltpu.make_async_remote_copy(
            src_ref=gqs.at[c, to],
            dst_ref=gq_ref.at[lanes(me), pl.ds(c * CHUNK, CHUNK)],
            send_sem=gq_s.at[c, to],
            recv_sem=gq_r.at[c, me],
            device_id={"aa": to},
            device_id_type=MESH,
        )

    def gq_arrival(c, sender):
        return pltpu.make_async_remote_copy(
            src_ref=gqs.at[c, sender],
            dst_ref=gq_ref.at[lanes(sender), pl.ds(c * CHUNK, CHUNK)],
            send_sem=gq_s.at[c, sender],
            recv_sem=gq_r.at[c, sender],
            device_id={"aa": sender},
            device_id_type=MESH,
        )

    def gq_local(c):
        return pltpu.make_async_copy(gqs.at[c, me], gq_ref.at[lanes(me), pl.ds(c * CHUNK, CHUNK)], own_sem.at[c])

    def pair_span(i):
        return pl.ds(pl.multiple_of(i * (2 * tok), CHUNK), 2 * tok)

    def pair_copy(i):
        return pltpu.make_async_remote_copy(
            src_ref=pair_out.at[pair_span(i)],
            dst_ref=pair_in.at[pair_span(i)],
            send_sem=pr_s.at[i],
            recv_sem=pr_r.at[i],
            device_id={"aa": partner},
            device_id_type=MESH,
        )

    def kv_cols(sender):
        return pl.ds(pl.multiple_of(lax.rem(sender, 2) * half + sender // 2 * HD, HD), HD)

    def kv_copy(to):
        return pltpu.make_async_remote_copy(
            src_ref=kvs.at[rows_of(to)],
            dst_ref=gkv_ref.at[:, kv_cols(me)],
            send_sem=kv_s.at[to],
            recv_sem=kv_r.at[me],
            device_id={"aa": to},
            device_id_type=MESH,
        )

    def kv_arrival(sender):
        return pltpu.make_async_remote_copy(
            src_ref=kvs.at[rows_of(sender)],
            dst_ref=gkv_ref.at[:, kv_cols(sender)],
            send_sem=kv_s.at[sender],
            recv_sem=kv_r.at[sender],
            device_id={"aa": sender},
            device_id_type=MESH,
        )

    def join(i):
        span = pair_span(i)
        pair_copy(i).wait_recv()

        @pl.when(odd == 0)
        def _():
            kvs[span, :] = (dvk_ref[span, HD:] * scaling + pair_in[span, :].astype(jnp.float32)).astype(jnp.bfloat16)

        @pl.when(odd == 1)
        def _():
            kvs[span, :] = (dvk_ref[span, 0:HD] + pair_in[span, :].astype(jnp.float32)).astype(jnp.bfloat16)

        for j in range(2):
            @pl.when(2 * i + j != me)
            def _():
                kv_copy(2 * i + j).start()

    def grads(c):
        final = c == chunks - 1

        def pair(step, carry):
            i = peers // 2 - 1 - step
            douts, queries, deltas = [], [], []
            for j in range(2):
                a = 2 * i + j

                @pl.when(a != me)
                def _():
                    dout_arrival(c, a).wait_recv()

                cols = slice(c * CHUNK, (c + 1) * CHUNK)
                dout = (drecv[c, a].astype(jnp.float32) * inv_ref[a, :, cols]).astype(jnp.bfloat16).astype(jnp.float32)
                deltas.append(jnp.sum(dout * ot_ref[a, :, cols], axis=0, keepdims=True))
                douts.append(dout)
                queries.append(qa[pl.ds(pl.multiple_of(a * tok + c * CHUNK, CHUNK), CHUNK), :])
            dout = jnp.concatenate(douts, axis=1)
            dout_low = dout.astype(jnp.bfloat16)
            dout_rows = dout.T.astype(jnp.bfloat16)
            delta = jnp.concatenate(deltas, axis=1)
            query = jnp.concatenate(queries, axis=0)

            def unit(u, grad_q):
                span = pair_span(u)
                p = p_ref[c, pair_rows(i, u * (2 * tok), 2 * tok), :]
                dp = jnp.dot(va[span, :], dout_low, preferred_element_type=jnp.float32)
                ds = (p.astype(jnp.float32) * (dp - delta)).astype(jnp.bfloat16)
                dvk_ref[span, 0:HD] += jnp.dot(p, dout_rows, preferred_element_type=jnp.float32)
                dvk_ref[span, HD:] += jnp.dot(ds, query, preferred_element_type=jnp.float32)
                return grad_q + jnp.dot(kt[:, span], ds, preferred_element_type=jnp.float32)

            grad_q = lax.fori_loop(0, i + 1, unit, jnp.zeros((HD, 2 * CHUNK), jnp.float32))
            for j in range(2):
                a = 2 * i + j
                gqs[c, a] = (grad_q[:, j * CHUNK : (j + 1) * CHUNK] * scaling).astype(jnp.bfloat16)

                @pl.when(a != me)
                def _():
                    gq_copy(c, a).start()

            if final:
                span = pair_span(i)

                @pl.when(odd == 0)
                def _():
                    pair_out[span, :] = dvk_ref[span, 0:HD].astype(jnp.bfloat16)

                @pl.when(odd == 1)
                def _():
                    pair_out[span, :] = (dvk_ref[span, HD:] * scaling).astype(jnp.bfloat16)

                pair_copy(i).start()

                @pl.when(step > 0)
                def _():
                    join(i + 1)

            return carry

        lax.fori_loop(0, peers // 2, pair, 0)
        gq_local(c).start()

    stats(0, 2)
    relay(0, 2)
    relay(2, 0)
    stats(2, 3)
    relay(1, 2)
    stats(3, peers // 2)
    relay(2, 1)
    weight_copy.wait()
    project_half(0, 0)
    project_half(0, 1)
    relay(2, 2)
    project_half(1, 0)
    project_half(2, 0)
    project_half(1, 1)
    grads(0)
    grads(1)
    project_half(2, 1)
    grads(2)

    join(0)
    kv_local = pltpu.make_async_copy(kvs.at[rows_of(me)], gkv_ref.at[:, kv_cols(me)], own_sem.at[3])
    kv_local.start()

    for c in range(chunks):
        gq_local(c).wait()
    kv_local.wait()
    for r in range(1, peers):
        other = peer(r)
        for c in range(chunks):
            gq_arrival(c, other).wait_recv()
        kv_arrival(other).wait_recv()
    for r in range(1, peers):
        other = peer(r)
        for kind in (0, 3):
            exchange(kind, other, me, r).wait_send()
        for c in range(chunks):
            dout_send(c, other).wait_send()
            gq_copy(c, other).wait_send()
        kv_copy(other).wait_send()
    for kind in (1, 2):
        exchange(kind, partner, me, 1).wait_send()
        for r in range(2, peers, 2):
            exchange(kind, peer(r), me, r).wait_send()
            forward(kind, peer(r), r).wait_send()
    for i in range(peers // 2):
        pair_copy(i).wait_send()
    for side in range(2):
        for s in range(last):
            @pl.when(gather_sends(side, s))
            def _(side=side, s=s):
                for c in range(chunks):
                    gather(side, c, s).wait_send()


def attention_grads(query, keys, values, segment_ids, grad_out, w_out, scaling):
    peers, planes = lax.axis_size("aa"), lax.axis_size("ba")
    tok = query.shape[0]
    chunks = tok // CHUNK
    total = peers * tok
    pairs = peers // 2
    low, full = jnp.bfloat16, jnp.float32
    return pl.pallas_call(
        functools.partial(attention_kernel, peers, planes, chunks, scaling),
        out_shape=[
            jax.ShapeDtypeStruct((query.shape[1], tok), low),
            jax.ShapeDtypeStruct((tok, 2 * keys.shape[1]), low),
        ],
        in_specs=[HBM] * 6,
        out_specs=[WHOLE, WHOLE],
        scratch_shapes=[
            pltpu.VMEM(w_out.shape, low),
            pltpu.VMEM((w_out.shape[1], tok), low),
            pltpu.VMEM((total, HD), low),
            pltpu.VMEM((total, HD), low),
            pltpu.VMEM((total, HD), low),
            pltpu.VMEM((HD, total), low),
            pltpu.VMEM((HD, total), low),
            pltpu.VMEM((peers, 1, tok), jnp.int32),
            pltpu.VMEM((peers, 1, tok), full),
            pltpu.VMEM((total, tok), full),
            pltpu.VMEM((chunks, pairs * (pairs + 1) * tok, 2 * CHUNK), low),
            pltpu.VMEM((peers, HD, tok), full),
            pltpu.VMEM((peers, 1, tok), full),
            pltpu.VMEM((total, 2 * HD), full),
            pltpu.VMEM((chunks, peers * HD, CHUNK), full),
            pltpu.VMEM((chunks, peers, HD, CHUNK), low),
            pltpu.VMEM((chunks, peers, HD, CHUNK), low),
            pltpu.VMEM((chunks, peers, HD, CHUNK), low),
            pltpu.VMEM((total, HD), low),
            pltpu.VMEM((total, HD), low),
            pltpu.VMEM((total, HD), low),
            pltpu.SemaphoreType.DMA,
            pltpu.SemaphoreType.DMA((5,)),
            pltpu.SemaphoreType.DMA((2, peers)),
            pltpu.SemaphoreType.DMA((2, chunks, planes - 1)),
            pltpu.SemaphoreType.DMA((2, chunks, planes - 1)),
            pltpu.SemaphoreType.DMA((4, peers)),
            pltpu.SemaphoreType.DMA((4, peers)),
            pltpu.SemaphoreType.DMA((chunks, peers)),
            pltpu.SemaphoreType.DMA((chunks, peers)),
            pltpu.SemaphoreType.DMA((chunks, peers)),
            pltpu.SemaphoreType.DMA((chunks, peers)),
            pltpu.SemaphoreType.DMA((pairs,)),
            pltpu.SemaphoreType.DMA((pairs,)),
            pltpu.SemaphoreType.DMA((peers,)),
            pltpu.SemaphoreType.DMA((peers,)),
        ],
        compiler_params=pltpu.CompilerParams(
            collective_id=0, has_side_effects=True, vmem_limit_bytes=60 * 1024 * 1024
        ),
        name="attention_grads",
    )(query, keys, values, segment_ids.reshape(1, -1), grad_out.T, w_out)


def local(query, keys, values, grad_out, segment_ids, w_query, w_key, w_value, w_out):
    seq_devices, planes = lax.axis_size("aa"), lax.axis_size("ba")
    heads, groups = query.shape[1] // HD, keys.shape[1] // HD
    fits = heads == seq_devices and 2 * groups == heads and planes == 4 and query.shape[0] == 3 * CHUNK
    if not fits:
        return local_ring(query, keys, values, grad_out, segment_ids, w_query, w_key, w_value, w_out)
    scaling = (D / HQ) ** (-0.5)
    grad_q, grad_kv = attention_grads(query, keys, values, segment_ids, grad_out, w_out, scaling)
    return project_scatter(grad_q, grad_kv, w_query, w_key, w_value).T


def solution(mesh):
    return jax.shard_map(
        local,
        mesh=mesh,
        in_specs=(
            P("aa", "ba"),
            P("aa", "ba"),
            P("aa", "ba"),
            P("aa", "ba"),
            P("aa"),
            P(None, "ba"),
            P(None, "ba"),
            P(None, "ba"),
            P("ba", None),
        ),
        out_specs=P("aa", "ba"),
        check_vma=False,
    )
```

```python
import functools

import jax
import jax.numpy as jnp
from jax import lax
from jax.experimental import pallas as pl
from jax.experimental.pallas import tpu as pltpu
from jax.sharding import PartitionSpec as P

D = 5376
HQ = 32
HD = 128
DOCS = 6


NEG_FILL = -1e30


def from_behind(value, axis, steps):
    count = lax.axis_size(axis)
    pairs = [(source, (source + steps) % count) for source in range(count)]
    return lax.ppermute(value, axis, pairs)


def block_scores(query, dout, keys, values, query_pos, query_seg, key_pos, key_seg, scaling):
    row_count = query.shape[0]
    col_count = keys.shape[0]
    groups = keys.shape[1] // HD
    query_four = query.reshape(row_count, groups, 2, HD)
    dout_four = dout.reshape(row_count, groups, 2, HD)
    key_three = keys.reshape(col_count, groups, HD)
    value_three = values.reshape(col_count, groups, HD)
    scores = (
        jnp.einsum("iagd,jad->agij", query_four, key_three, preferred_element_type=jnp.float32)
        * scaling
    )
    dprobs = jnp.einsum(
        "iagd,jad->agij", dout_four, value_three, preferred_element_type=jnp.float32
    )
    allowed = (key_pos[None, :] <= query_pos[:, None]) & (key_seg[None, :] == query_seg[:, None])
    return (scores, dprobs, allowed, query_four, dout_four, key_three)


def forward_stats(
    query, dout, keys, values, query_pos, query_seg, key_pos, key_seg, scaling, state
):
    run_max, run_sum, run_dot = state
    scores, dprobs, allowed, unused_q, unused_d, unused_k = block_scores(
        query, dout, keys, values, query_pos, query_seg, key_pos, key_seg, scaling
    )
    masked = jnp.where(allowed, scores, NEG_FILL)
    new_max = jnp.maximum(run_max, jnp.max(masked, axis=-1))
    expo = jnp.where(allowed, jnp.exp(scores - new_max[..., None]), 0.0)
    return (new_max, jnp.sum(expo, axis=-1), jnp.sum(expo * dprobs, axis=-1))


def block_grads(
    query, dout, row_lse, row_delta, keys, values, query_pos, query_seg, key_pos, key_seg, scaling
):
    scores, dprobs, allowed, query_four, dout_four, key_three = block_scores(
        query, dout, keys, values, query_pos, query_seg, key_pos, key_seg, scaling
    )
    softmax_w = jnp.where(allowed, jnp.exp(scores - row_lse[..., None]), 0.0)
    dscores = softmax_w * (dprobs - row_delta[..., None])
    softmax_low = softmax_w.astype(jnp.bfloat16)
    dscores_low = dscores.astype(jnp.bfloat16)
    grad_v = jnp.einsum(
        "agij,iagd->jad", softmax_low, dout_four, preferred_element_type=jnp.float32
    )
    grad_k = (
        jnp.einsum("agij,iagd->jad", dscores_low, query_four, preferred_element_type=jnp.float32)
        * scaling
    )
    grad_q = (
        jnp.einsum("agij,jad->iagd", dscores_low, key_three, preferred_element_type=jnp.float32)
        * scaling
    )
    return (
        grad_q.reshape(query.shape[0], -1),
        grad_k.reshape(keys.shape[0], -1),
        grad_v.reshape(keys.shape[0], -1),
    )


def project_back(grad, weight):
    return lax.dot_general(
        grad, weight, (((1,), (1,)), ((), ())), preferred_element_type=jnp.float32
    )


def local_ring(query, keys, values, grad_out, segment_ids, w_query, w_key, w_value, w_out):
    seq_devices = lax.axis_size("aa")
    own_index = lax.axis_index("aa")
    tok_count = query.shape[0]
    scaling = (D / HQ) ** (-0.5)
    groups = keys.shape[1] // HD
    all_seg = lax.all_gather(segment_ids, "aa", axis=0, tiled=True)
    dout = project_back(lax.all_gather(grad_out, "ba", axis=1, tiled=True), w_out).astype(
        jnp.bfloat16
    )
    offsets = lax.iota(jnp.int32, tok_count)
    own_pos = own_index * tok_count + offsets
    own_seg = lax.dynamic_slice_in_dim(all_seg, own_index * tok_count, tok_count)
    stat_shape = (groups, 2, tok_count)
    stats_start = (
        jnp.full(stat_shape, NEG_FILL, jnp.float32),
        jnp.zeros(stat_shape, jnp.float32),
        jnp.zeros(stat_shape, jnp.float32),
    )
    piece = (
        lax.all_gather(keys, "aa", axis=0, tiled=True),
        lax.all_gather(values, "aa", axis=0, tiled=True),
    )
    width = piece[0].shape[0]
    key_pos = lax.iota(jnp.int32, width)
    key_seg = all_seg
    run_max, run_sum, run_dot = forward_stats(
        query, dout, piece[0], piece[1], own_pos, own_seg, key_pos, key_seg, scaling, stats_start
    )
    row_lse = run_max + jnp.log(run_sum)
    row_delta = run_dot / run_sum
    zero_q = jnp.zeros(query.shape, jnp.float32)
    zero_k = jnp.zeros(keys.shape, jnp.float32)

    def step_keys(step_index, state):
        (keys_now, values_now), (dk_now, dv_now), grad_q = state
        anchor = (own_index - step_index) % seq_devices
        key_pos = anchor * tok_count + offsets
        key_seg = lax.dynamic_slice_in_dim(all_seg, anchor * tok_count, tok_count)
        add_q, add_k, add_v = block_grads(
            query,
            dout,
            row_lse,
            row_delta,
            keys_now,
            values_now,
            own_pos,
            own_seg,
            key_pos,
            key_seg,
            scaling,
        )
        bundle_next = from_behind((keys_now, values_now), "aa", 1)
        sums_next = (
            from_behind((dk_now + add_k).astype(jnp.bfloat16), "aa", 1).astype(jnp.float32),
            from_behind((dv_now + add_v).astype(jnp.bfloat16), "aa", 1).astype(jnp.float32),
        )
        return (bundle_next, sums_next, grad_q + add_q)

    initial = ((keys, values), (zero_k, zero_k), zero_q)
    final = lax.fori_loop(0, seq_devices, step_keys, initial)
    grad_q = final[2]
    grad_k = final[1][0]
    grad_v = final[1][1]
    partial_value = (
        project_back(grad_q.astype(jnp.bfloat16), w_query)
        + project_back(grad_k.astype(jnp.bfloat16), w_key)
        + project_back(grad_v.astype(jnp.bfloat16), w_value)
    )
    return lax.psum_scatter(
        partial_value.astype(jnp.bfloat16), "ba", scatter_dimension=1, tiled=True
    )


def fold_rows(value, op):
    return op(value.reshape(-1, 8, value.shape[1]), axis=0)


CONTRACT_LAST = (((1,), (1,)), ((), ()))


WHOLE = pl.BlockSpec(memory_space=pltpu.VMEM)


MESH = pl.DeviceIdType.MESH
HBM = pl.BlockSpec(memory_space=pl.ANY)
SUBS = 3


def scatter_kernel(planes, gq_ref, gkv_ref, wq_ref, wk_ref, wv_ref, out_ref, wqb, wkb, wvb, sbuf, rbuf, total_ref, wsem, ssem, rsem):
    z = lax.axis_index("ba")
    barrier = pltpu.get_barrier_semaphore()
    last = planes - 1
    low = z > 0
    high = z < last

    @pl.when(low)
    def _():
        pl.semaphore_signal(barrier, inc=1, device_id={"ba": z - 1}, device_id_type=MESH)

    @pl.when(high)
    def _():
        pl.semaphore_signal(barrier, inc=1, device_id={"ba": z + 1}, device_id_type=MESH)

    rows = out_ref.shape[0]
    sub_rows = rows // SUBS

    def target(side, step):
        return jnp.where(side == 0, step, last - step)

    near = jnp.where(2 * z > last, 0, 1)
    sides = (near, 1 - near)
    counts = (jnp.maximum(z, last - z), jnp.minimum(z, last - z))

    def weight_copies(feature, sub):
        source = pl.ds(pl.multiple_of(feature * rows + sub * sub_rows, 16), sub_rows)
        span = pl.ds(sub * sub_rows, sub_rows)
        return [
            pltpu.make_async_copy(src.at[source], dst.at[feature, span], wsem.at[feature, sub, part])
            for part, (src, dst) in enumerate(((wq_ref, wqb), (wk_ref, wkb), (wv_ref, wvb)))
        ]

    def load(feature, subs):
        for sub in subs:
            for copy in weight_copies(feature, sub):
                copy.start()

    def await_weights(feature, sub):
        for copy in weight_copies(feature, sub):
            copy.wait()

    load(target(near, 0), range(1))
    load(target(near, 0), range(1, SUBS))

    def load_rest():
        for step in range(last):
            for which in range(2):
                if (which, step) == (0, 0):
                    continue

                @pl.when(step < counts[which])
                def _(step=step, which=which):
                    load(target(sides[which], step), range(SUBS))
        load(z, range(SUBS))

    pl.semaphore_wait(barrier, jnp.minimum(z, 1) + jnp.minimum(last - z, 1))

    half = gkv_ref.shape[1] // 2

    def part(slot, sub):
        span = pl.ds(sub * sub_rows, sub_rows)
        acc = jnp.dot(wqb[slot, span, :], gq_ref[...], preferred_element_type=jnp.float32)
        acc += lax.dot_general(wkb[slot, span, :], gkv_ref[:, 0:half], CONTRACT_LAST, preferred_element_type=jnp.float32)
        return acc + lax.dot_general(wvb[slot, span, :], gkv_ref[:, half:], CONTRACT_LAST, preferred_element_type=jnp.float32)

    def hop(side, step, sub):
        span = pl.ds(sub * sub_rows, sub_rows)
        return pltpu.make_async_remote_copy(
            src_ref=sbuf.at[side, step, span],
            dst_ref=rbuf.at[side, step, span],
            send_sem=ssem.at[side, step, sub],
            recv_sem=rsem.at[side, step, sub],
            device_id={"ba": jnp.where(side == 0, z - 1, z + 1)},
            device_id_type=MESH,
        )

    inner = low & high
    order = sorted(
        [(step * SUBS + sub + 2 * which * (step + 1) - 0.5 * which, which, step, sub)
         for which in range(2) for step in range(last - which) for sub in range(SUBS)]
    )
    for _unused, which, step, sub in order:
        @pl.when(step < counts[which])
        def _(which=which, step=step, sub=sub):
            side = sides[which]
            feature = target(side, step)
            await_weights(feature, sub)
            if (which, step, sub) == (0, 0, 0):
                load_rest()
            span = pl.ds(sub * sub_rows, sub_rows)
            acc = part(feature, sub)

            @pl.when(inner)
            def _():
                hop(side, step, sub).wait_recv()
                sbuf[side, step, span, :] = (acc + rbuf[side, step, span, :].astype(jnp.float32)).astype(jnp.bfloat16)

            @pl.when(jnp.logical_not(inner))
            def _():
                sbuf[side, step, span, :] = acc.astype(jnp.bfloat16)

            hop(side, step, sub).start()

    for sub in range(SUBS):
        await_weights(z, sub)
    for sub in range(SUBS):
        span = pl.ds(sub * sub_rows, sub_rows)
        total_ref[span, :] = part(z, sub)
    for sub in range(SUBS):
        span = pl.ds(sub * sub_rows, sub_rows)
        for side in range(2):
            for step in range(last):
                here = (z == target(side, step)) & (high if side == 0 else low)

                @pl.when(here)
                def _(side=side, step=step):
                    hop(side, step, sub).wait_recv()
                    total_ref[span, :] += rbuf[side, step, span, :].astype(jnp.float32)

        out_ref[span, :] = total_ref[span, :].astype(jnp.bfloat16)

    for which in range(2):
        for step in range(last):
            @pl.when(step < counts[which])
            def _(which=which, step=step):
                for sub in range(SUBS):
                    hop(sides[which], step, sub).wait_send()


def project_scatter(gq, gkv, w_query, w_key, w_value):
    planes = lax.axis_size("ba")
    rows = w_query.shape[0] // planes
    tokens = gq.shape[1]
    last = planes - 1
    return pl.pallas_call(
        functools.partial(scatter_kernel, planes),
        out_shape=jax.ShapeDtypeStruct((rows, tokens), jnp.bfloat16),
        in_specs=[WHOLE, WHOLE, HBM, HBM, HBM],
        out_specs=WHOLE,
        scratch_shapes=[
            pltpu.VMEM((planes, rows, w_query.shape[1]), jnp.bfloat16),
            pltpu.VMEM((planes, rows, w_key.shape[1]), jnp.bfloat16),
            pltpu.VMEM((planes, rows, w_value.shape[1]), jnp.bfloat16),
            pltpu.VMEM((2, last, rows, tokens), jnp.bfloat16),
            pltpu.VMEM((2, last, rows, tokens), jnp.bfloat16),
            pltpu.VMEM((rows, tokens), jnp.float32),
            pltpu.SemaphoreType.DMA((planes, SUBS, 3)),
            pltpu.SemaphoreType.DMA((2, last, SUBS)),
            pltpu.SemaphoreType.DMA((2, last, SUBS)),
        ],
        compiler_params=pltpu.CompilerParams(
            collective_id=1, has_side_effects=True, vmem_limit_bytes=56 * 1024 * 1024
        ),
        name="project_scatter",
    )(gq, gkv, w_query, w_key, w_value)


CHUNK = 128
LOG2E = 1.4426950408889634


def attention_kernel(peers, planes, chunks, scaling, q_ref, k_ref, v_ref, seg_ref, g_ref, w_ref, gq_ref, gkv_ref,
                     wbuf, fbuf, qa, ka, va, kt, vt, segs, starts_ref, s_ref, p_ref, ot_ref, inv_ref, dvk_ref, acc_ref,
                     dsend, drecv, gqs, pair_out, pair_in, kvs,
                     local_sem, own_sem, f_s, ag_s, ag_r, x_s, x_r, d_s, d_r, gq_s, gq_r, pr_s, pr_r, kv_s, kv_r):
    me = lax.axis_index("aa")
    z = lax.axis_index("ba")
    last = planes - 1
    tok = q_ref.shape[0]
    feats = g_ref.shape[0]
    half = gkv_ref.shape[1] // 2
    barrier = pltpu.get_barrier_semaphore()

    def lanes(index):
        return pl.ds(pl.multiple_of(index * HD, HD), HD)

    def rows_of(index):
        return pl.ds(pl.multiple_of(index * tok, tok), tok)

    def peer(r):
        return lax.rem(me + r, peers)

    for r in range(1, peers):
        pl.semaphore_signal(barrier, inc=1, device_id={"aa": peer(r)}, device_id_type=MESH)
    for r in range(1, planes):
        pl.semaphore_signal(barrier, inc=1, device_id={"ba": lax.rem(z + r, planes)}, device_id_type=MESH)

    def own_copies():
        return [
            pltpu.make_async_copy(g_ref, fbuf.at[pl.ds(pl.multiple_of(z * feats, 16), feats)], own_sem.at[0]),
            pltpu.make_async_copy(q_ref.at[:, lanes(me)], qa.at[rows_of(me)], own_sem.at[1]),
            pltpu.make_async_copy(k_ref.at[:, lanes(me // 2)], ka.at[rows_of(me)], own_sem.at[2]),
            pltpu.make_async_copy(v_ref.at[:, lanes(me // 2)], va.at[rows_of(me)], own_sem.at[3]),
        ]

    weight_copy = pltpu.make_async_copy(w_ref, wbuf, local_sem)
    for copy in own_copies():
        copy.start()
    segs[me] = seg_ref[...].reshape(1, tok)
    pl.semaphore_wait(barrier, peers + planes - 2)

    def gather(side, c, s):
        source = z - s if side == 0 else z + s
        span = pl.ds(pl.multiple_of(source * feats, 16), feats)
        cols = pl.ds(c * CHUNK, CHUNK)
        return pltpu.make_async_remote_copy(
            src_ref=g_ref.at[:, cols] if s == 0 else fbuf.at[span, cols],
            dst_ref=fbuf.at[span, cols],
            send_sem=ag_s.at[side, c, s],
            recv_sem=ag_r.at[side, c, s],
            device_id={"ba": z + 1 if side == 0 else z - 1},
            device_id_type=MESH,
        )

    def arrival(side, c, s):
        source = z - 1 - s if side == 0 else z + 1 + s
        span = pl.ds(pl.multiple_of(source * feats, 16), feats)
        cols = pl.ds(c * CHUNK, CHUNK)
        return pltpu.make_async_remote_copy(
            src_ref=fbuf.at[span, cols],
            dst_ref=fbuf.at[span, cols],
            send_sem=ag_s.at[side, c, s],
            recv_sem=ag_r.at[side, c, s],
            device_id={"ba": z + 1 if side == 0 else z - 1},
            device_id_type=MESH,
        )

    def gather_sends(side, s):
        return (z >= s) & (z < last) if side == 0 else (z + s <= last) & (z > 0)

    def relay(c, s):
        for side in range(2):
            @pl.when(gather_sends(side, s))
            def _(side=side):
                if s > 0:
                    arrival(side, c, s - 1).wait_recv()
                gather(side, c, s).start()

    def finish_gather(c, steps):
        for side in range(2):
            for s in steps:
                @pl.when((z == last) if side == 0 else (z == 0))
                def _(side=side, s=s):
                    arrival(side, c, s).wait_recv()

    odd = lax.rem(me, 2)
    partner = me + 1 - 2 * odd

    def forward(kind, sender, r):
        land = (ka if kind == 1 else va).at[rows_of(sender)]
        return pltpu.make_async_remote_copy(
            src_ref=land,
            dst_ref=land,
            send_sem=f_s.at[kind - 1, r],
            recv_sem=x_r.at[kind, sender],
            device_id={"aa": partner},
            device_id_type=MESH,
        )

    def exchange(kind, to, sender, peer_sem):
        shard = (q_ref.at[:, lanes(to)], k_ref.at[:, lanes(to // 2)], v_ref.at[:, lanes(to // 2)], segs.at[me])[kind]
        land = (qa.at[rows_of(sender)], ka.at[rows_of(sender)], va.at[rows_of(sender)], segs.at[sender])[kind]
        return pltpu.make_async_remote_copy(
            src_ref=shard,
            dst_ref=land,
            send_sem=x_s.at[kind, peer_sem],
            recv_sem=x_r.at[kind, sender],
            device_id={"aa": to},
            device_id_type=MESH,
        )

    relay(0, 0)
    relay(1, 0)
    for r in range(1, peers):
        exchange(3, peer(r), me, r).start()
    for r in range(1, peers):
        exchange(0, peer(r), me, r).start()
    for kind in (1, 2):
        exchange(kind, partner, me, 1).start()
        for r in range(2, peers, 2):
            exchange(kind, peer(r), me, r).start()
    weight_copy.start()
    dvk_ref[...] = jnp.zeros_like(dvk_ref)
    relay(0, 1)
    relay(1, 1)
    for copy in own_copies():
        copy.wait()
    for r in range(1, peers):
        exchange(3, me, peer(r), r).wait_recv()

    ids = segs[...]
    starts = jnp.zeros(ids.shape, jnp.float32)
    for doc in range(1, DOCS):
        before = jnp.sum(jnp.where(ids < doc, 1.0, 0.0), axis=(0, 2), keepdims=True)
        starts = jnp.where(ids == doc, before, starts)
    starts_ref[...] = starts
    for kind in (1, 2):
        for r in range(2, peers, 2):
            exchange(kind, me, peer(r), r).wait_recv()
            forward(kind, peer(r), r).start()

    def pair_rows(i, at, size):
        return pl.ds(pl.multiple_of(i * (i + 1) * tok + at, CHUNK), size)

    def stats(start, stop):
        def block(i, j):
            a = 2 * i + j

            @pl.when(a != me)
            def _():
                exchange(0, me, a, 0).wait_recv()

            @pl.when(lax.rem(a + me, 2) == 1)
            def _():
                for kind in (1, 2):
                    exchange(kind, me, a, 0).wait_recv()

            kt[:, rows_of(a)] = ka[rows_of(a), :].astype(jnp.float32).T.astype(jnp.bfloat16)
            vt[:, rows_of(a)] = va[rows_of(a), :].astype(jnp.float32).T.astype(jnp.bfloat16)
            query = qa[rows_of(a), :]
            begin = starts_ref[a]

            def scores(u, diagonal):
                s = lax.dot_general(ka[rows_of(u), :], query, CONTRACT_LAST, preferred_element_type=jnp.float32)
                key = lax.broadcasted_iota(jnp.int32, (tok, tok), 0)
                allowed = (key + u * tok).astype(jnp.float32) >= begin
                if diagonal:
                    allowed &= key <= lax.broadcasted_iota(jnp.int32, (tok, tok), 1)
                s = jnp.where(allowed, s * (scaling * LOG2E), NEG_FILL)
                s_ref[rows_of(u), :] = s
                return fold_rows(s, jnp.max)

            top = lax.fori_loop(0, a, lambda u, t: jnp.maximum(t, scores(u, False)),
                                jnp.full((8, tok), NEG_FILL, jnp.float32))
            top = jnp.max(jnp.maximum(top, scores(a, True)), axis=0, keepdims=True)

            def weights(u, state):
                total, out = state
                p = jnp.exp2(s_ref[rows_of(u), :] - top)
                low = p.astype(jnp.bfloat16)
                for c in range(chunks):
                    p_ref[c, pair_rows(i, u * tok, tok), j * CHUNK : (j + 1) * CHUNK] = low[:, c * CHUNK : (c + 1) * CHUNK]
                return (total + fold_rows(p, jnp.sum),
                        out + jnp.dot(vt[:, rows_of(u)], low, preferred_element_type=jnp.float32))

            state = (jnp.zeros((8, tok), jnp.float32), jnp.zeros((HD, tok), jnp.float32))
            total, out = lax.fori_loop(0, a + 1, weights, state)
            inverse = 1.0 / jnp.sum(total, axis=0, keepdims=True)
            inv_ref[a] = inverse
            ot_ref[a] = out * inverse
            if j == 0:
                for c in range(chunks):
                    p_ref[c, pair_rows(i, (a + 1) * tok, tok), 0:CHUNK] = jnp.zeros((tok, CHUNK), jnp.bfloat16)

        def pair(i, carry):
            block(i, 0)
            block(i, 1)
            return carry

        lax.fori_loop(start, stop, pair, 0)

    def dout_send(c, to):
        return pltpu.make_async_remote_copy(
            src_ref=dsend.at[c, to],
            dst_ref=drecv.at[c, me],
            send_sem=d_s.at[c, to],
            recv_sem=d_r.at[c, me],
            device_id={"aa": to},
            device_id_type=MESH,
        )

    def dout_arrival(c, sender):
        return pltpu.make_async_remote_copy(
            src_ref=dsend.at[c, sender],
            dst_ref=drecv.at[c, sender],
            send_sem=d_s.at[c, sender],
            recv_sem=d_r.at[c, sender],
            device_id={"aa": sender},
            device_id_type=MESH,
        )

    depth = planes // 2 * feats
    near = z // (planes // 2)

    def project_half(c, which):
        side = near if which == 0 else 1 - near
        span = pl.ds(pl.multiple_of(side * depth, CHUNK), depth)
        finish_gather(c, range(1) if which == 0 else range(1, last))
        group = peers // 2

        def heads(i, carry):
            rows = pl.ds(pl.multiple_of(i * (group * HD), HD), group * HD)
            out = jnp.dot(wbuf[rows, span], fbuf[span, c * CHUNK : (c + 1) * CHUNK], preferred_element_type=jnp.float32)
            if which == 0:
                acc_ref[c, rows, :] = out
                return carry
            out += acc_ref[c, rows, :]
            for j in range(group):
                to = i * group + j
                dsend[c, to] = out[j * HD : (j + 1) * HD, :].astype(jnp.bfloat16)

                @pl.when(to != me)
                def _():
                    dout_send(c, to).start()

            return carry

        lax.fori_loop(0, peers // group, heads, 0)
        if which == 1:
            drecv[c, me] = dsend[c, me]

    def gq_copy(c, to):
        return pltpu.make_async_remote_copy(
            src_ref=gqs.at[c, to],
            dst_ref=gq_ref.at[lanes(me), pl.ds(c * CHUNK, CHUNK)],
            send_sem=gq_s.at[c, to],
            recv_sem=gq_r.at[c, me],
            device_id={"aa": to},
            device_id_type=MESH,
        )

    def gq_arrival(c, sender):
        return pltpu.make_async_remote_copy(
            src_ref=gqs.at[c, sender],
            dst_ref=gq_ref.at[lanes(sender), pl.ds(c * CHUNK, CHUNK)],
            send_sem=gq_s.at[c, sender],
            recv_sem=gq_r.at[c, sender],
            device_id={"aa": sender},
            device_id_type=MESH,
        )

    def gq_local(c):
        return pltpu.make_async_copy(gqs.at[c, me], gq_ref.at[lanes(me), pl.ds(c * CHUNK, CHUNK)], own_sem.at[c])

    def pair_span(i):
        return pl.ds(pl.multiple_of(i * (2 * tok), CHUNK), 2 * tok)

    def pair_copy(i):
        return pltpu.make_async_remote_copy(
            src_ref=pair_out.at[pair_span(i)],
            dst_ref=pair_in.at[pair_span(i)],
            send_sem=pr_s.at[i],
            recv_sem=pr_r.at[i],
            device_id={"aa": partner},
            device_id_type=MESH,
        )

    def kv_cols(sender):
        return pl.ds(pl.multiple_of(lax.rem(sender, 2) * half + sender // 2 * HD, HD), HD)

    def kv_copy(to):
        return pltpu.make_async_remote_copy(
            src_ref=kvs.at[rows_of(to)],
            dst_ref=gkv_ref.at[:, kv_cols(me)],
            send_sem=kv_s.at[to],
            recv_sem=kv_r.at[me],
            device_id={"aa": to},
            device_id_type=MESH,
        )

    def kv_arrival(sender):
        return pltpu.make_async_remote_copy(
            src_ref=kvs.at[rows_of(sender)],
            dst_ref=gkv_ref.at[:, kv_cols(sender)],
            send_sem=kv_s.at[sender],
            recv_sem=kv_r.at[sender],
            device_id={"aa": sender},
            device_id_type=MESH,
        )

    def join(i):
        span = pair_span(i)
        pair_copy(i).wait_recv()

        @pl.when(odd == 0)
        def _():
            kvs[span, :] = (dvk_ref[span, HD:] * scaling + pair_in[span, :].astype(jnp.float32)).astype(jnp.bfloat16)

        @pl.when(odd == 1)
        def _():
            kvs[span, :] = (dvk_ref[span, 0:HD] + pair_in[span, :].astype(jnp.float32)).astype(jnp.bfloat16)

        for j in range(2):
            @pl.when(2 * i + j != me)
            def _():
                kv_copy(2 * i + j).start()

    def grads(c):
        final = c == chunks - 1

        def pair(step, carry):
            i = peers // 2 - 1 - step
            douts, queries, deltas = [], [], []
            for j in range(2):
                a = 2 * i + j

                @pl.when(a != me)
                def _():
                    dout_arrival(c, a).wait_recv()

                cols = slice(c * CHUNK, (c + 1) * CHUNK)
                dout = (drecv[c, a].astype(jnp.float32) * inv_ref[a, :, cols]).astype(jnp.bfloat16).astype(jnp.float32)
                deltas.append(jnp.sum(dout * ot_ref[a, :, cols], axis=0, keepdims=True))
                douts.append(dout)
                queries.append(qa[pl.ds(pl.multiple_of(a * tok + c * CHUNK, CHUNK), CHUNK), :])
            dout = jnp.concatenate(douts, axis=1)
            dout_low = dout.astype(jnp.bfloat16)
            dout_rows = dout.T.astype(jnp.bfloat16)
            delta = jnp.concatenate(deltas, axis=1)
            query = jnp.concatenate(queries, axis=0)

            def unit(u, grad_q):
                span = pair_span(u)
                p = p_ref[c, pair_rows(i, u * (2 * tok), 2 * tok), :]
                dp = jnp.dot(va[span, :], dout_low, preferred_element_type=jnp.float32)
                ds = (p.astype(jnp.float32) * (dp - delta)).astype(jnp.bfloat16)
                dvk_ref[span, 0:HD] += jnp.dot(p, dout_rows, preferred_element_type=jnp.float32)
                dvk_ref[span, HD:] += jnp.dot(ds, query, preferred_element_type=jnp.float32)
                return grad_q + jnp.dot(kt[:, span], ds, preferred_element_type=jnp.float32)

            grad_q = lax.fori_loop(0, i + 1, unit, jnp.zeros((HD, 2 * CHUNK), jnp.float32))
            for j in range(2):
                a = 2 * i + j
                gqs[c, a] = (grad_q[:, j * CHUNK : (j + 1) * CHUNK] * scaling).astype(jnp.bfloat16)

                @pl.when(a != me)
                def _():
                    gq_copy(c, a).start()

            if final:
                span = pair_span(i)

                @pl.when(odd == 0)
                def _():
                    pair_out[span, :] = dvk_ref[span, 0:HD].astype(jnp.bfloat16)

                @pl.when(odd == 1)
                def _():
                    pair_out[span, :] = (dvk_ref[span, HD:] * scaling).astype(jnp.bfloat16)

                pair_copy(i).start()

                @pl.when(step > 0)
                def _():
                    join(i + 1)

            return carry

        lax.fori_loop(0, peers // 2, pair, 0)
        gq_local(c).start()

    stats(0, 2)
    relay(0, 2)
    relay(2, 0)
    stats(2, 3)
    relay(1, 2)
    stats(3, peers // 2)
    relay(2, 1)
    weight_copy.wait()
    project_half(0, 0)
    project_half(0, 1)
    relay(2, 2)
    project_half(1, 0)
    project_half(2, 0)
    project_half(1, 1)
    grads(0)
    grads(1)
    project_half(2, 1)
    grads(2)

    join(0)
    kv_local = pltpu.make_async_copy(kvs.at[rows_of(me)], gkv_ref.at[:, kv_cols(me)], own_sem.at[3])
    kv_local.start()

    for c in range(chunks):
        gq_local(c).wait()
    kv_local.wait()
    for r in range(1, peers):
        other = peer(r)
        for c in range(chunks):
            gq_arrival(c, other).wait_recv()
        kv_arrival(other).wait_recv()
    for r in range(1, peers):
        other = peer(r)
        for kind in (0, 3):
            exchange(kind, other, me, r).wait_send()
        for c in range(chunks):
            dout_send(c, other).wait_send()
            gq_copy(c, other).wait_send()
        kv_copy(other).wait_send()
    for kind in (1, 2):
        exchange(kind, partner, me, 1).wait_send()
        for r in range(2, peers, 2):
            exchange(kind, peer(r), me, r).wait_send()
            forward(kind, peer(r), r).wait_send()
    for i in range(peers // 2):
        pair_copy(i).wait_send()
    for side in range(2):
        for s in range(last):
            @pl.when(gather_sends(side, s))
            def _(side=side, s=s):
                for c in range(chunks):
                    gather(side, c, s).wait_send()


def attention_grads(query, keys, values, segment_ids, grad_out, w_out, scaling):
    peers, planes = lax.axis_size("aa"), lax.axis_size("ba")
    tok = query.shape[0]
    chunks = tok // CHUNK
    total = peers * tok
    pairs = peers // 2
    low, full = jnp.bfloat16, jnp.float32
    return pl.pallas_call(
        functools.partial(attention_kernel, peers, planes, chunks, scaling),
        out_shape=[
            jax.ShapeDtypeStruct((query.shape[1], tok), low),
            jax.ShapeDtypeStruct((tok, 2 * keys.shape[1]), low),
        ],
        in_specs=[HBM, HBM, HBM, WHOLE, HBM, HBM],
        out_specs=[WHOLE, WHOLE],
        scratch_shapes=[
            pltpu.VMEM(w_out.shape, low),
            pltpu.VMEM((w_out.shape[1], tok), low),
            pltpu.VMEM((total, HD), low),
            pltpu.VMEM((total, HD), low),
            pltpu.VMEM((total, HD), low),
            pltpu.VMEM((HD, total), low),
            pltpu.VMEM((HD, total), low),
            pltpu.VMEM((peers, 1, tok), jnp.int32),
            pltpu.VMEM((peers, 1, tok), full),
            pltpu.VMEM((total, tok), full),
            pltpu.VMEM((chunks, pairs * (pairs + 1) * tok, 2 * CHUNK), low),
            pltpu.VMEM((peers, HD, tok), full),
            pltpu.VMEM((peers, 1, tok), full),
            pltpu.VMEM((total, 2 * HD), full),
            pltpu.VMEM((chunks, peers * HD, CHUNK), full),
            pltpu.VMEM((chunks, peers, HD, CHUNK), low),
            pltpu.VMEM((chunks, peers, HD, CHUNK), low),
            pltpu.VMEM((chunks, peers, HD, CHUNK), low),
            pltpu.VMEM((total, HD), low),
            pltpu.VMEM((total, HD), low),
            pltpu.VMEM((total, HD), low),
            pltpu.SemaphoreType.DMA,
            pltpu.SemaphoreType.DMA((5,)),
            pltpu.SemaphoreType.DMA((2, peers)),
            pltpu.SemaphoreType.DMA((2, chunks, planes - 1)),
            pltpu.SemaphoreType.DMA((2, chunks, planes - 1)),
            pltpu.SemaphoreType.DMA((4, peers)),
            pltpu.SemaphoreType.DMA((4, peers)),
            pltpu.SemaphoreType.DMA((chunks, peers)),
            pltpu.SemaphoreType.DMA((chunks, peers)),
            pltpu.SemaphoreType.DMA((chunks, peers)),
            pltpu.SemaphoreType.DMA((chunks, peers)),
            pltpu.SemaphoreType.DMA((pairs,)),
            pltpu.SemaphoreType.DMA((pairs,)),
            pltpu.SemaphoreType.DMA((peers,)),
            pltpu.SemaphoreType.DMA((peers,)),
        ],
        compiler_params=pltpu.CompilerParams(
            collective_id=0, has_side_effects=True, vmem_limit_bytes=60 * 1024 * 1024
        ),
        name="attention_grads",
    )(query, keys, values, segment_ids, grad_out.T, w_out)


def local(query, keys, values, grad_out, segment_ids, w_query, w_key, w_value, w_out):
    seq_devices, planes = lax.axis_size("aa"), lax.axis_size("ba")
    heads, groups = query.shape[1] // HD, keys.shape[1] // HD
    fits = heads == seq_devices and 2 * groups == heads and planes == 4 and query.shape[0] == 3 * CHUNK
    if not fits:
        return local_ring(query, keys, values, grad_out, segment_ids, w_query, w_key, w_value, w_out)
    scaling = (D / HQ) ** (-0.5)
    grad_q, grad_kv = attention_grads(query, keys, values, segment_ids, grad_out, w_out, scaling)
    return project_scatter(grad_q, grad_kv, w_query, w_key, w_value).T


def solution(mesh):
    return jax.shard_map(
        local,
        mesh=mesh,
        in_specs=(
            P("aa", "ba"),
            P("aa", "ba"),
            P("aa", "ba"),
            P("aa", "ba"),
            P("aa"),
            P(None, "ba"),
            P(None, "ba"),
            P(None, "ba"),
            P("ba", None),
        ),
        out_specs=P("aa", "ba"),
        check_vma=False,
    )
```
